128 devices in a mesh: gx: 8 (over z_lo, x), gy: 16 (over z_hi, y, core).
Axes of the slice: x: 4, y: 4, z: 4 (z_hi: 2, z_lo: 2; z = z_hi * 2 + z_lo), core: 2. Of those that a mesh axis runs over, the one named last changes fastest.
Arguments:
- e_field: float32 [3, 256, 512, 128], P(None, 'gx', 'gy'), may hold values from -6 to 6
- h_field: float32 [3, 256, 512, 128], P(None, 'gx', 'gy'), may hold values from -6 to 6
- psi: float32 [12, 256, 512, 128], P(None, 'gx', 'gy'), may hold values from -6 to 6
- material: int32 [256, 512, 128], P('gx', 'gy'), may hold values from 0 to 7
- eps_table: float32 [8], replicated, may hold values from 1 to 1.2
- sigma_table: float32 [8], replicated, may hold values from 0 to 0.05
Outputs:
- e_out: float32 [3, 256, 512, 128], P(None, 'gx', 'gy')
- h_out: float32 [3, 256, 512, 128], P(None, 'gx', 'gy')
- psi_out: float32 [12, 256, 512, 128], P(None, 'gx', 'gy')
The draws below stay inside these ranges and needn't reach their ends.
All inputs are finite; a program needn't handle non-finite values.
Results may differ from the reference program's by a relative error of at most 0.0003.
Values sent between devices are 32-bit elements; how exact they have to be, the bound alone decides.
A program may use at most 128 MiB of HBM per device.

```python
import math
import jax
import jax.numpy as jnp
from jax import lax

NZ = 128
PML = 16
STEPS = 16
NMAT = 8
NX = 256
NY = 512


def place_ends(array, stream_key, smallest, high):
    longest = array.shape.index(max(array.shape))
    spots = []
    for shift in (0, 1):
        where = [jax.random.randint(jax.random.fold_in(stream_key, axis), (), 0, length) for axis, length in enumerate(array.shape)]
        where[longest] = (where[longest] + shift) % array.shape[longest]
        spots.append(tuple(where))
    return array.at[spots[0]].set(smallest).at[spots[1]].set(high)


def block_scale(own_key, shape, pieces, least, top_value):
    gain = 1.0
    for dim, parts in pieces:
        heights = jax.random.uniform(jax.random.fold_in(jax.random.fold_in(own_key, 6), dim), (parts,), jnp.float32, least / len(pieces), top_value / len(pieces))
        gain = gain * jnp.repeat(jnp.exp(heights), shape[dim] // parts).reshape((-1,) + (1,) * (len(shape) - 1 - dim))
    return gain


def normal_values(stream_key, dims, spread, reach, cuts=(), kind=jnp.bfloat16):
    result = jax.random.normal(stream_key, dims, jnp.float32) * spread
    if len(cuts) > 0:
        result = block_scale(stream_key, dims, cuts, -0.22, 0.18) * result
    return jnp.clip(result, min=-reach, max=reach).astype(kind)


def setup_inputs(seed: int = 0) -> dict:
    seeds = jax.random.split(jax.random.key(seed), 7)
    e_field = normal_values(seeds[0], (3, NX, NY, NZ), 1.0, 6.0, ((1, 8), (2, 16)), jnp.float32)
    h_field = normal_values(seeds[1], (3, NX, NY, NZ), 1.0, 6.0, ((1, 8), (2, 16)), jnp.float32)
    psi = normal_values(seeds[2], (12, NX, NY, NZ), 1.0, 6.0, ((1, 8), (2, 16)), jnp.float32)
    material = place_ends(jax.random.randint(seeds[3], (NX, NY, NZ), 0, NMAT), jax.random.fold_in(seeds[3], 1), 0, NMAT - 1).astype(jnp.int32)
    eps_table = jnp.clip(jnp.exp(jax.random.uniform(seeds[4], (NMAT,), jnp.float32, math.log(1.0), math.log(1.2))), 1.0, 1.2)
    sigma_table = jnp.clip(jax.random.uniform(seeds[5], (NMAT,), jnp.float32, 0.0, 0.05), 0.0, 0.05)
    return {"e_field": e_field, "h_field": h_field, "psi": psi, "material": material, "eps_table": eps_table, "sigma_table": sigma_table}


time_step = 0.5
sigma_peak = 3.0
kappa_peak = 5.0
alpha_peak = 0.05
curl_table = (((2, 1), (1, 2)), ((0, 2), (2, 0)), ((1, 0), (0, 1)))


def profile(length, offset, extent, shift_half, thickness):
    position = (offset + lax.iota(jnp.int32, length)).astype(jnp.float32) + shift_half
    slab_width = jnp.float32(thickness)
    depth_frac = jnp.maximum(jnp.maximum((slab_width - position) / slab_width, (position - (extent - slab_width)) / slab_width), 0.0)
    depth_cube = depth_frac * depth_frac * depth_frac
    sigma_value = sigma_peak * depth_cube
    kappa_value = 1.0 + (kappa_peak - 1.0) * depth_cube
    alpha_value = alpha_peak * (1.0 - depth_frac)
    decays = jnp.exp(-(sigma_value / kappa_value + alpha_value) * time_step)
    scaling = sigma_value * (decays - 1.0) / (kappa_value * (sigma_value + kappa_value * alpha_value))
    inside_slab = depth_frac > 0.0
    return jnp.where(inside_slab, decays, 0.0), jnp.where(inside_slab, scaling, 0.0), 1.0 / kappa_value


def shaped(vector, direction):
    target_shape = [1, 1, 1]
    target_shape[direction] = vector.shape[0]
    return vector.reshape(target_shape)


def forward(field, direction, following):
    shifted = lax.slice_in_dim(field, 1, field.shape[direction], axis=direction)
    return jnp.concatenate([shifted, following], axis=direction) - field


def backward(field, direction, preceding):
    shifted = lax.slice_in_dim(field, 0, field.shape[direction] - 1, axis=direction)
    return field - jnp.concatenate([preceding, shifted], axis=direction)


def zero_layer(field, direction):
    return jnp.zeros_like(lax.slice_in_dim(field, 0, 1, axis=direction))


def update_term(difference, auxiliary, coefficient, direction):
    decays, scaling, inverse = coefficient
    renewed = decays * auxiliary + scaling * difference
    return inverse * difference + renewed, renewed


def curl(difference_of, auxiliary, first_slot, coefficients, renew):
    results = []
    renewed_list = []
    for component in range(3):
        plus_pair, minus_pair = curl_table[component]
        slot = first_slot + 2 * component
        plus_value, plus_aux = renew(difference_of(plus_pair[0], plus_pair[1]), auxiliary[slot], coefficients[plus_pair[1]], plus_pair[1])
        minus_value, minus_aux = renew(difference_of(minus_pair[0], minus_pair[1]), auxiliary[slot + 1], coefficients[minus_pair[1]], minus_pair[1])
        results.append(plus_value - minus_value)
        renewed_list.append(plus_aux)
        renewed_list.append(minus_aux)
    return results, renewed_list


def material_coefficients(material, eps_table, sigma_table):
    losses = sigma_table * time_step / (2.0 * eps_table)
    keep_table = (1.0 - losses) / (1.0 + losses)
    drive_table = (time_step / eps_table) / (1.0 + losses)
    keeping = jnp.zeros(material.shape, jnp.float32)
    driving = jnp.zeros(material.shape, jnp.float32)
    for number in range(NMAT):
        chosen = material == number
        keeping = keeping + jnp.where(chosen, keep_table[number], 0.0)
        driving = driving + jnp.where(chosen, drive_table[number], 0.0)
    return keeping, driving


def reference(e_field, h_field, psi, material, eps_table, sigma_table):
    extents = (NX, NY, NZ)
    magnetic_coef = [tuple(shaped(vector, direction) for vector in profile(extents[direction], 0, extents[direction], 0.5, PML)) for direction in range(3)]
    electric_coef = [tuple(shaped(vector, direction) for vector in profile(extents[direction], 0, extents[direction], 0.0, PML)) for direction in range(3)]
    keeping, driving = material_coefficients(material, eps_table, sigma_table)

    def advance(turn_index, carry):
        electric, magnetic, auxiliary = carry

        def electric_ahead(source, direction):
            field = electric[source]
            return forward(field, direction, zero_layer(field, direction))

        curl_h, renewed_h = curl(electric_ahead, auxiliary, 0, magnetic_coef, update_term)
        magnetic_new = jnp.stack([magnetic[component] - time_step * curl_h[component] for component in range(3)])

        def magnetic_behind(source, direction):
            field = magnetic_new[source]
            return backward(field, direction, zero_layer(field, direction))

        curl_e, renewed_e = curl(magnetic_behind, auxiliary, 6, electric_coef, update_term)
        electric_new = jnp.stack([keeping * electric[component] + driving * curl_e[component] for component in range(3)])
        return (electric_new, magnetic_new, jnp.stack(renewed_h + renewed_e))

    e_out, h_out, psi_out = lax.fori_loop(0, STEPS, advance, (e_field, h_field, psi))
    return (e_out, h_out, psi_out)
```

```python
import functools

import jax
import jax.numpy as jnp
from jax import lax
from jax.experimental import pallas as pl
from jax.experimental.pallas import tpu as pltpu
from jax.sharding import PartitionSpec as P

PML = 16
STEPS = 16
NMAT = 8
time_step = 0.5
sigma_peak = 3.0
kappa_peak = 5.0
alpha_peak = 0.05

M = 4
XO, XR = 5, 42
YO, YP = 8, 48
PYP = 24
U = 4
NA = 7
Z_SLOTS = (1, 2, 7, 8)
X_SLOTS = (3, 4, 9, 10)
Y_SLOTS = (0, 5, 6, 11)
MESH = pl.DeviceIdType.MESH
DIRS = ((-1, 0), (1, 0), (0, -1), (0, 1), (-1, -1), (-1, 1), (1, -1), (1, 1))
OPP = (1, 0, 3, 2, 7, 6, 5, 4)
LAYER = NA * 32
FACE = M * LAYER
CORNER = NA * M * M
EDGE = M * 4 * 16


def profile_of(position, extent):
    width = jnp.float32(PML)
    depth = jnp.maximum(
        jnp.maximum((width - position) / width, (position - (extent - width)) / width), 0.0
    )
    cube = depth * depth * depth
    sigma = sigma_peak * cube
    kappa = 1.0 + (kappa_peak - 1.0) * cube
    alpha = alpha_peak * (1.0 - depth)
    b = jnp.exp(-(sigma / kappa + alpha) * time_step)
    a = sigma * (b - 1.0) / (kappa * (sigma + kappa * alpha))
    inside = depth > 0.0
    return jnp.where(inside, b, 0.0), jnp.where(inside, a, 0.0), 1.0 / kappa


def kernel(nx, ny, e_in, h_in, psi_in, mat_in, eps_in, sig_in, e_out, h_out, psi_out, *scratch):
    scratch = list(scratch)
    take = lambda n: [scratch.pop(0) for _ in range(n)]
    E, H, PZ, PX, PY = take(3), take(3), take(4), take(4), take(4)
    KP, DR, MF, MI, ZB = take(5)
    xtab, ytab, ztab = take(1)[0], take(1)[0], take(1)[0]
    send_f, recv_f = take(4), take(4)
    send_c, recv_c = take(4), take(4)
    send_e, recv_e = take(4), take(4)
    send_m, recv_m = take(4), take(4)
    send_mc, recv_mc = take(4), take(4)
    in_sem, out_sem, zero_sem, s_sem, r_sem, sm_sem, rm_sem = take(7)

    gx, gy = lax.axis_index("gx"), lax.axis_index("gy")
    zero = jnp.minimum(gx, 0)
    x_first, x_last = gx == 0, gx == nx - 1
    y_first, y_last = gy == 0, gy == ny - 1
    x_edge = jnp.logical_or(x_first, x_last)
    y_edge = jnp.logical_or(y_first, y_last)
    exists = []
    for dx, dy in DIRS:
        ok = None
        for delta, first, last in ((dx, x_first, x_last), (dy, y_first, y_last)):
            if delta:
                here = jnp.logical_not(first if delta < 0 else last)
                ok = here if ok is None else jnp.logical_and(ok, here)
        exists.append(ok)
    pxbase = jnp.where(x_first, 0, 16)
    pybase = jnp.where(y_first, -4, 12)
    view = lambda ref: ref.reshape(XR, YP, 128)
    tile = lambda ref: view(ref).at[pl.ds(XO, 32), pl.ds(YO, 32), :]
    pxview = lambda ref: ref.reshape(16, YP, 128).at[:, pl.ds(YO, 32), :]
    pyrows = lambda ref: ref.reshape(XR, PYP, 128).at[pl.ds(XO, 32), pl.ds(4, 16), :]

    loads = [(h_in.at[c], tile(H[c])) for c in range(3)]
    loads += [(e_in.at[c], tile(E[c])) for c in range(3)]
    loads += [(psi_in.at[s], tile(PZ[k])) for k, s in enumerate(Z_SLOTS)]
    loads += [(mat_in, MI)]
    loads = [pltpu.make_async_copy(a, b, in_sem.at[i]) for i, (a, b) in enumerate(loads)]
    for copy in loads:
        copy.start()
    xloads = [
        pltpu.make_async_copy(
            psi_in.at[s, pl.ds(pxbase, 16)], pxview(PX[k]), in_sem.at[12 + k]
        )
        for k, s in enumerate(X_SLOTS)
    ]
    py_local = pl.multiple_of(pybase + 4, 8)
    yloads = [
        pltpu.make_async_copy(
            psi_in.at[s, :, pl.ds(py_local, 16)], pyrows(PY[k]), in_sem.at[16 + k]
        )
        for k, s in enumerate(Y_SLOTS)
    ]

    @pl.when(x_edge)
    def _():
        for copy in xloads:
            copy.start()

    @pl.when(y_edge)
    def _():
        for copy in yloads:
            copy.start()

    barrier = pltpu.get_barrier_semaphore()
    count = 0
    for d, (dx, dy) in enumerate(DIRS):
        count = count + exists[d].astype(jnp.int32)

        @pl.when(exists[d])
        def _(dx=dx, dy=dy):
            pl.semaphore_signal(barrier, inc=1, device_id=(gx + dx, gy + dy), device_id_type=MESH)

    row = lax.broadcasted_iota(jnp.int32, (8, 128), 0)
    lane = lax.broadcasted_iota(jnp.int32, (8, 128), 1)
    zeros = jnp.zeros((8, 128), jnp.float32)
    for half, shift in ((0, 0.5), (1, 0.0)):
        for k, value in enumerate(profile_of(lane.astype(jnp.float32) + shift, 128)):
            ztab[(half * 3 + k) * 8 : (half * 3 + k) * 8 + 8, :] = value
        for i in range(6):
            for tab, offset, extent in (
                (xtab, gx * 32 - XO, nx * 32),
                (ytab, gy * 32 - YO, ny * 32),
            ):
                position = (row + (i * 8 + offset)).astype(jnp.float32) + shift
                for k, value in enumerate(profile_of(position, extent)):
                    at = (half * 3 + k) * 48 + i * 8
                    tab[at : at + 8, :] = value

    def clear(i, c):
        for k in range(4):
            ZB[pl.ds(pl.multiple_of(i * 32 + k * 8, 8), 8), :] = zeros
        return c

    lax.fori_loop(0, 32, clear, 0)
    for ref in E + H:
        for x in (0, 1, 2, 3, 4, 37, 38, 39, 40, 41):
            for k in range(6):
                ref[x * YP + k * 8 : x * YP + k * 8 + 8, :] = zeros

    def clear_rim(i, c):
        base = pl.multiple_of((i + XO) * YP, 8)
        for ref in E + H:
            ref[pl.ds(base, 8), :] = zeros
            ref[pl.ds(base + 40, 8), :] = zeros
        return c

    lax.fori_loop(0, 32, clear_rim, 0)

    zb3 = ZB.reshape(32, 32, 128)
    x_rest = jnp.where(x_first, 16, 0)
    y_rest = pl.multiple_of(jnp.where(y_first, 16, 0), 8)
    zx_all = [pltpu.make_async_copy(zb3, psi_out.at[s], zero_sem.at[k]) for k, s in enumerate(X_SLOTS)]
    zx_half = [
        pltpu.make_async_copy(zb3.at[pl.ds(0, 16)], psi_out.at[s, pl.ds(x_rest, 16)], zero_sem.at[k])
        for k, s in enumerate(X_SLOTS)
    ]
    zy_all = [
        pltpu.make_async_copy(zb3, psi_out.at[s], zero_sem.at[4 + k]) for k, s in enumerate(Y_SLOTS)
    ]
    zy_half = [
        pltpu.make_async_copy(
            zb3.at[:, pl.ds(0, 16)], psi_out.at[s, :, pl.ds(y_rest, 16)], zero_sem.at[4 + k]
        )
        for k, s in enumerate(Y_SLOTS)
    ]

    def zero_fill(act):
        for edge, whole, half in ((x_edge, zx_all, zx_half), (y_edge, zy_all, zy_half)):

            @pl.when(edge)
            def _(half=half):
                for copy in half:
                    act(copy)

            @pl.when(jnp.logical_not(edge))
            def _(whole=whole):
                for copy in whole:
                    act(copy)

    for copy in loads:
        copy.wait()

    @pl.when(x_edge)
    def _():
        for copy in xloads:
            copy.wait()

    @pl.when(y_edge)
    def _():
        for copy in yloads:
            copy.wait()

    zero_fill(lambda copy: copy.start())

    keep_of, drive_of = [], []
    for n in range(NMAT):
        eps = jnp.full((8, 128), eps_in[n], jnp.float32)
        loss = jnp.full((8, 128), sig_in[n], jnp.float32) * time_step / (2.0 * eps)
        keep_of.append((1.0 - loss) / (1.0 + loss))
        drive_of.append((time_step / eps) / (1.0 + loss))

    def choose(bits, table):
        for bit in bits:
            table = [jnp.where(bit, table[i + 1], table[i]) for i in range(0, len(table), 2)]
        return table[0]

    def coefficients(base):
        number = MF[pl.ds(base, 8), :].astype(jnp.int32)
        bits = [(number & (1 << k)) != 0 for k in range(3)]
        KP[pl.ds(base, 8), :] = choose(bits, keep_of)
        DR[pl.ds(base, 8), :] = choose(bits, drive_of)

    at = lambda x, y: (x + XO) * YP + YO + y

    def own_material(x, c):
        for k in range(4):
            MF[pl.ds(at(x, 8 * k), 8), :] = MI[
                pl.ds(pl.multiple_of(x * 32 + 8 * k, 8), 8), :
            ].astype(jnp.float32)
            coefficients(at(x, 8 * k))
        return c

    lax.fori_loop(0, 32, own_material, 0)
    pl.semaphore_wait(barrier, count)

    def remote(d, src, dst, ssem, rsem):
        dx, dy = DIRS[d]
        return pltpu.make_async_remote_copy(
            src_ref=src,
            dst_ref=dst,
            send_sem=ssem,
            recv_sem=rsem,
            device_id=(gx + dx, gy + dy),
            device_id_type=MESH,
        )

    def guarded(d, *copies):
        @pl.when(exists[d])
        def _():
            for copy in copies:
                copy.start()

    def layer_rows(d, layer, q, low):
        if low is None:
            place = layer if DIRS[d][d // 2] < 0 else 31 - layer
        else:
            place = -1 - layer if DIRS[d][d // 2] < 0 else 32 + layer
        if d < 2:
            return pl.ds(at(place, 8 * q) + zero, 8)
        return pl.ds(at(8 * q, place) + zero, 8, stride=YP)

    def pack(parts):
        out = pltpu.roll(parts[3], 112, 1)
        for s in (2, 1, 0):
            out = jnp.where(lane < 32 * (s + 1), pltpu.roll(parts[s], 32 * s + 16, 1), out)
        return out

    def send_face(d, blk):
        buf = send_f[d]

        def one(layer, c):
            for q in range(4):
                rows = layer_rows(d, layer, q, None)
                for k, ref in enumerate(E + H):
                    buf[pl.ds(pl.multiple_of(layer * LAYER + k * 32 + q * 8, 8), 8), :] = ref[
                        rows, :
                    ]
                buf[pl.ds(pl.multiple_of(layer * LAYER + 192 + q * 8, 8), 8), :] = pack(
                    [ref[rows, :] for ref in PZ]
                )
            return c

        lax.fori_loop(0, M, one, 0)
        guarded(d, remote(d, buf, recv_f[OPP[d]].at[blk], s_sem.at[d, 0], r_sem.at[blk, OPP[d], 0]))

    def send_corner(d, blk):
        buf, (dx, dy) = send_c[d - 4], DIRS[d]
        ys = 0 if dy < 0 else 28
        for i in range(M):
            x = i if dx < 0 else 31 - i
            rows = pl.ds(at(x, ys) + zero, 8)
            for k, value in enumerate(
                [ref[rows, :] for ref in E + H] + [pack([ref[rows, :] for ref in PZ])]
            ):
                buf[k * 16 + i * 4 : k * 16 + i * 4 + 4, :] = value[0:4, :]
        copy = remote(
            d, buf, recv_c[OPP[d] - 4].at[blk], s_sem.at[d, 0], r_sem.at[blk, OPP[d], 0]
        )
        guarded(d, copy)

    def edge_rows(d, layer, low):
        if low is None:
            place = layer if DIRS[d][d // 2] < 0 else 31 - layer
        else:
            place = -1 - layer if DIRS[d][d // 2] < 0 else 32 + layer
        if d < 2:
            return [pl.ds((place + XO) * PYP + 4 + 8 * q + zero, 8) for q in range(2)]
        return [pl.ds(8 * q * YP + YO + place + zero, 8, stride=YP) for q in range(2)]

    def send_edge(d, blk):
        @pl.when(jnp.logical_and(exists[d], y_edge if d < 2 else x_edge))
        def _():
            buf = send_e[d]
            for layer in range(M):
                for k, ref in enumerate(PY if d < 2 else PX):
                    for q, rows in enumerate(edge_rows(d, layer, None)):
                        s = layer * 64 + k * 16 + q * 8
                        buf[s : s + 8, :] = ref[rows, :]
            remote(
                d, buf, recv_e[OPP[d]].at[blk], s_sem.at[d, 1], r_sem.at[blk, OPP[d], 1]
            ).start()

    def receive_face(d, blk):
        @pl.when(exists[d])
        def _():
            buf = recv_f[d]
            copy = remote(d, send_f[d], buf.at[blk], s_sem.at[d, 0], r_sem.at[blk, d, 0])
            copy.wait_recv()
            copy.wait_send()

            def unpack(layer, c):
                for q in range(4):
                    rows = layer_rows(d, layer, q, True)
                    for k, ref in enumerate(E + H):
                        ref[rows, :] = buf[
                            blk, pl.ds(pl.multiple_of(layer * LAYER + k * 32 + q * 8, 8), 8), :
                        ]
                    packed = buf[
                        blk, pl.ds(pl.multiple_of(layer * LAYER + 192 + q * 8, 8), 8), :
                    ]
                    for s, ref in enumerate(PZ):
                        ref[rows, :] = pltpu.roll(packed, 112 - 32 * s, 1)
                return c

            lax.fori_loop(0, M, unpack, 0)

    def receive_corner(d, blk):
        @pl.when(exists[d])
        def _():
            buf, (dx, dy) = recv_c[d - 4], DIRS[d]
            copy = remote(d, send_c[d - 4], buf.at[blk], s_sem.at[d, 0], r_sem.at[blk, d, 0])
            copy.wait_recv()
            copy.wait_send()
            ys = -4 if dy < 0 else 32
            for i in range(M):
                x = -1 - i if dx < 0 else 32 + i
                rows = pl.ds(at(x, ys) + zero, 4)
                for k, ref in enumerate(E + H):
                    ref[rows, :] = buf[blk, k * 16 + i * 4 : k * 16 + i * 4 + 4, :]
                packed = buf[blk, 96 + i * 4 : 96 + i * 4 + 4, :]
                for s, ref in enumerate(PZ):
                    ref[rows, :] = pltpu.roll(packed, 112 - 32 * s, 1)

    def receive_edge(d, blk):
        @pl.when(jnp.logical_and(exists[d], y_edge if d < 2 else x_edge))
        def _():
            buf = recv_e[d]
            copy = remote(d, send_e[d], buf.at[blk], s_sem.at[d, 1], r_sem.at[blk, d, 1])
            copy.wait_recv()
            copy.wait_send()
            for layer in range(M):
                for k, ref in enumerate(PY if d < 2 else PX):
                    for q, rows in enumerate(edge_rows(d, layer, True)):
                        s = layer * 64 + k * 16 + q * 8
                        ref[rows, :] = buf[blk, s : s + 8, :]

    for d in range(4):
        for layer in range(M):
            for q in range(4):
                s = layer * 32 + q * 8
                send_m[d][s : s + 8, :] = MF[layer_rows(d, layer, q, None), :]
        guarded(d, remote(d, send_m[d], recv_m[OPP[d]], sm_sem.at[d], rm_sem.at[OPP[d]]))
    for d in range(4, 8):
        dx, dy = DIRS[d]
        for i in range(M):
            rows = pl.ds(at(i if dx < 0 else 31 - i, 0 if dy < 0 else 28) + zero, 4)
            send_mc[d - 4][i * 4 : i * 4 + 4, :] = MF[rows, :]
        guarded(
            d, remote(d, send_mc[d - 4], recv_mc[OPP[d] - 4], sm_sem.at[d], rm_sem.at[OPP[d]])
        )

    def receive_material():
        for x in (0, 1, 2, 3, 4, 37, 38, 39, 40, 41):
            for k in range(6):
                MF[x * YP + k * 8 : x * YP + k * 8 + 8, :] = zeros

        def clear_side(x, c):
            MF[pl.ds(pl.multiple_of((x + XO) * YP, 8), 8), :] = zeros
            MF[pl.ds(pl.multiple_of((x + XO) * YP + 40, 8), 8), :] = zeros
            return c

        lax.fori_loop(0, 32, clear_side, 0)
        for d in range(8):

            @pl.when(exists[d])
            def _(d=d):
                dx, dy = DIRS[d]
                if d < 4:
                    copy = remote(d, send_m[d], recv_m[d], sm_sem.at[d], rm_sem.at[d])
                else:
                    copy = remote(d, send_mc[d - 4], recv_mc[d - 4], sm_sem.at[d], rm_sem.at[d])
                copy.wait_recv()
                copy.wait_send()
                for i in range(M):
                    if d < 4:
                        for q in range(4):
                            s = i * 32 + q * 8
                            MF[layer_rows(d, i, q, True), :] = recv_m[d][s : s + 8, :]
                    else:
                        x = -1 - i if dx < 0 else 32 + i
                        rows = pl.ds(at(x, -4 if dy < 0 else 32) + zero, 4)
                        MF[rows, :] = recv_mc[d - 4][i * 4 : i * 4 + 4, :]

        def whole_row(x, c):
            for k in range(5):
                coefficients(at(x, 8 * k - 4) + zero)
            return c

        def ends_of_row(x, c):
            for k in (0, 4):
                coefficients(at(x, 8 * k - 4) + zero)
            return c

        lax.fori_loop(-4, 0, whole_row, 0)
        lax.fori_loop(32, 36, whole_row, 0)
        lax.fori_loop(0, 32, ends_of_row, 0)

    def table(tab, half, k, start, n):
        return tab[pl.ds(half * 3 * n + k * n + start, 8), :]

    def half_step(half, g, starts, mask_of, px, py):
        source, target = (E, H) if half == 0 else (H, E)
        step = 1 if half == 0 else -1
        zc = [ztab[(half * 3 + k) * 8 : (half * 3 + k) * 8 + 8, :] for k in range(3)]
        keep_lane = lane < 127 if half == 0 else lane > 0
        for r in range(U):
            x = g * U - U + r
            if px:
                xc = [
                    jnp.broadcast_to(xtab[pl.ds((half * 3 + k) * 48 + x + XO, 1), :], (8, 128))
                    for k in range(3)
                ]
            for i, y in enumerate(starts):
                rows = lambda dx, dy: pl.ds(at(x + dx, y + dy) + zero, 8)
                here = rows(0, 0)
                mask = mask_of(r, x, i)

                def put(ref, where, value):
                    pltpu.store(ref.at[where, :], value, mask=mask)

                def diff(a, b):
                    return a - b if half == 0 else b - a

                s0, s1, s2 = (ref[here, :] for ref in source)
                sh = 127 if half == 0 else 1
                turn = lambda v: jnp.where(keep_lane, pltpu.roll(v, sh, 1), 0.0)
                dz1, dz0 = diff(turn(s1), s1), diff(turn(s0), s0)
                dy2 = diff(source[2][rows(0, step), :], s2)
                dy0 = diff(source[0][rows(0, step), :], s0)
                dx2 = diff(source[2][rows(step, 0), :], s2)
                dx1 = diff(source[1][rows(step, 0), :], s1)

                def term(d, coef, ref, where):
                    b, a, q = coef
                    new = b * ref[where, :] + a * d
                    put(ref, where, new)
                    return q * d + new

                tz1 = term(dz1, zc, PZ[2 * half], here)
                tz0 = term(dz0, zc, PZ[2 * half + 1], here)
                if px:
                    there = pl.ds((x - pxbase) * YP + YO + y + zero, 8)
                    tx2 = term(dx2, xc, PX[2 * half], there)
                    tx1 = term(dx1, xc, PX[2 * half + 1], there)
                else:
                    tx2, tx1 = dx2, dx1
                if i in py:
                    yc = [
                        ytab[pl.ds((half * 3 + k) * 48 + YO + y + zero, 8), :] for k in range(3)
                    ]
                    there = pl.ds((x + XO) * PYP + (y - py[i]) + zero, 8)
                    ty2 = term(dy2, yc, PY[2 * half], there)
                    ty0 = term(dy0, yc, PY[2 * half + 1], there)
                else:
                    ty2, ty0 = dy2, dy0
                curls = (ty2 - tz1, tz0 - tx2, tx1 - ty0)
                if half == 0:
                    for ref, c in zip(target, curls):
                        put(ref, here, ref[here, :] - time_step * c)
                else:
                    kp, dr = KP[here, :], DR[here, :]
                    for ref, c in zip(target, curls):
                        put(ref, here, kp * ref[here, :] + dr * c)

    px0 = jnp.where(x_first, 1, jnp.where(x_last, 5, 0))
    px1 = jnp.where(x_first, 5, jnp.where(x_last, 9, 0))

    def groups(half, ga, gb, starts, mask_of, py):
        def plain(part, c):
            first = jnp.where(part == 0, ga, jnp.maximum(ga, px1))
            last = jnp.where(part == 0, jnp.minimum(gb, px0), gb)

            def one(g, c):
                half_step(half, g, starts, mask_of, False, py)
                return c

            return lax.fori_loop(first, last, one, c)

        lax.fori_loop(0, 2, plain, 0)

        def layered(g, c):
            half_step(half, g, starts, mask_of, True, py)
            return c

        lax.fori_loop(jnp.maximum(ga, px0), jnp.minimum(gb, px1), layered, 0)

    def by_place(run, low, high):
        @pl.when(y_first)
        def _():
            run({i: -4 for i in low})

        @pl.when(y_last)
        def _():
            run({i: 12 for i in high})

        @pl.when(jnp.logical_not(y_edge))
        def _():
            run({})

    def inner_range(t, half, first, last):
        lo = jnp.where(first, 0, t - 1 + half)
        hi = jnp.where(last, 32, 32 - t)
        return lo, hi

    def within(v, lo, hi):
        return jnp.logical_and(v >= lo, v < hi)

    starts_a = (0, 8, 16, 24)
    starts_b = (-4, 4, 12, 20, 28)

    def pass_a(t, py):
        for half in range(2):
            xlo, xhi = inner_range(t, half, x_first, x_last)
            ylo, yhi = inner_range(t, half, y_first, y_last)

            def mask_of(r, x, i, xlo=xlo, xhi=xhi, ylo=ylo, yhi=yhi):
                ok = within(x, xlo, xhi).astype(jnp.int32)
                if i in (0, 3):
                    return within(row + starts_a[i], ylo, jnp.where(ok > 0, yhi, -99))
                return row >= 8 - 8 * ok

            groups(half, 1, 9, starts_a, mask_of, py)

    def pass_b(t, py):
        g0 = jnp.where(x_first, 1, 0)
        g1 = jnp.where(x_last, 9, 10)
        ya = jnp.where(y_first, 0, -99)
        yb = jnp.where(y_last, 32, 99)
        for half in range(2):
            xc, xd = inner_range(t, half, x_first, x_last)
            yc, yd = inner_range(t, half, y_first, y_last)

            def mask_of(r, x, i, xc=xc, xd=xd, yc=yc, yd=yd):
                inner = within(x, xc, xd)
                if i not in (0, 4):
                    return row >= 8 * inner.astype(jnp.int32)
                y = row + starts_b[i]
                if i == 0:
                    return within(y, ya, jnp.where(inner, yc, 99))
                return within(y, jnp.where(inner, yd, -99), yb)

            def ends_mask(r, x, i, yc=yc, yd=yd):
                y = row + (-4 if i == 0 else 28)
                return within(y, ya, yc) if i == 0 else within(y, yd, yb)

            def part(p, c, half=half, mask_of=mask_of):
                first = jnp.where(p == 0, g0, 8)
                groups(half, first, jnp.where(p == 0, 2, g1), starts_b, mask_of, py)
                return c

            lax.fori_loop(0, 2, part, 0)
            ends_py = {k // 4: v for k, v in py.items() if k in (0, 4)}
            groups(half, 2, 8, (-4, 28), ends_mask, ends_py)

    def block(turn, c):
        blk = turn % 2
        for d in (0, 1, 2, 3):
            send_face(d, blk)
        for d in range(4, 8):
            send_corner(d, blk)
        for d in range(4):
            send_edge(d, blk)

        def step_a(t, c):
            by_place(lambda py: pass_a(t, py), (0, 1), (2, 3))
            return c

        lax.fori_loop(1, M + 1, step_a, 0)

        @pl.when(turn == 0)
        def _():
            receive_material()

        for d in range(4, 8):
            receive_corner(d, blk)
        for d in range(4):
            receive_edge(d, blk)
        for d in (2, 3, 0, 1):
            receive_face(d, blk)

        def step_b(t, c):
            by_place(lambda py: pass_b(t, py), (0, 1, 2), (2, 3, 4))
            return c

        lax.fori_loop(1, M + 1, step_b, 0)
        return c

    lax.fori_loop(0, STEPS // M, block, 0)

    zero_fill(lambda copy: copy.wait())
    stores = [(tile(E[c]), e_out.at[c]) for c in range(3)]
    stores += [(tile(H[c]), h_out.at[c]) for c in range(3)]
    stores += [(tile(PZ[k]), psi_out.at[s]) for k, s in enumerate(Z_SLOTS)]
    stores = [pltpu.make_async_copy(a, b, out_sem.at[i]) for i, (a, b) in enumerate(stores)]
    xstores = [
        pltpu.make_async_copy(pxview(PX[k]), psi_out.at[s, pl.ds(pxbase, 16)], out_sem.at[12 + k])
        for k, s in enumerate(X_SLOTS)
    ]
    ystores = [
        pltpu.make_async_copy(pyrows(PY[k]), psi_out.at[s, :, pl.ds(py_local, 16)], out_sem.at[16 + k])
        for k, s in enumerate(Y_SLOTS)
    ]

    def finish(act):
        for copy in stores:
            act(copy)

        @pl.when(x_edge)
        def _():
            for copy in xstores:
                act(copy)

        @pl.when(y_edge)
        def _():
            for copy in ystores:
                act(copy)

    finish(lambda copy: copy.start())
    finish(lambda copy: copy.wait())


def solution(mesh):
    nx, ny = mesh.shape["gx"], mesh.shape["gy"]
    f32 = jnp.float32
    field = P(None, "gx", "gy", None)

    def shards(e_field, h_field, psi, material, eps_table, sigma_table):
        big = pltpu.VMEM((XR * YP, 128), f32)
        dma = pltpu.SemaphoreType.DMA
        scratch = [big] * 10
        scratch += [pltpu.VMEM((16 * YP, 128), f32)] * 4
        scratch += [pltpu.VMEM((XR * PYP, 128), f32)] * 4
        scratch += [big, big, big, pltpu.VMEM((1024, 128), jnp.int32), pltpu.VMEM((1024, 128), f32)]
        scratch += [pltpu.VMEM((6 * 48, 128), f32)] * 2 + [pltpu.VMEM((48, 128), f32)]
        scratch += [pltpu.VMEM((FACE, 128), f32)] * 4 + [pltpu.VMEM((2, FACE, 128), f32)] * 4
        scratch += [pltpu.VMEM((CORNER, 128), f32)] * 4 + [pltpu.VMEM((2, CORNER, 128), f32)] * 4
        scratch += [pltpu.VMEM((EDGE, 128), f32)] * 4 + [pltpu.VMEM((2, EDGE, 128), f32)] * 4
        scratch += [pltpu.VMEM((128, 128), f32)] * 8 + [pltpu.VMEM((16, 128), f32)] * 8
        scratch += [
            dma((20,)),
            dma((20,)),
            dma((8,)),
            dma((8, 2)),
            dma((2, 8, 2)),
            dma((8,)),
            dma((8,)),
        ]
        anywhere = pl.BlockSpec(memory_space=pl.ANY)
        smem = pl.BlockSpec(memory_space=pltpu.SMEM)
        return pl.pallas_call(
            functools.partial(kernel, nx, ny),
            out_shape=(
                jax.ShapeDtypeStruct(e_field.shape, f32),
                jax.ShapeDtypeStruct(h_field.shape, f32),
                jax.ShapeDtypeStruct(psi.shape, f32),
            ),
            in_specs=[anywhere] * 4 + [smem] * 2,
            out_specs=(anywhere,) * 3,
            scratch_shapes=scratch,
            compiler_params=pltpu.CompilerParams(collective_id=0, has_side_effects=True),
        )(e_field, h_field, psi, material.reshape(1024, 128), eps_table, sigma_table)

    return jax.shard_map(
        shards,
        mesh=mesh,
        in_specs=(field, field, field, P("gx", "gy", None), P(), P()),
        out_specs=(field, field, field),
        check_vma=False,
    )
```

```python
import functools

import jax
import jax.numpy as jnp
from jax import lax
from jax.experimental import pallas as pl
from jax.experimental.pallas import tpu as pltpu
from jax.sharding import PartitionSpec as P

PML = 16
STEPS = 16
NMAT = 8
time_step = 0.5
sigma_peak = 3.0
kappa_peak = 5.0
alpha_peak = 0.05

M = 4
D = 2
PXR = 24
XO, XR = 5, 42
YO, YP = 8, 48
PYP = 24
U = 4
NA = 7
Z_SLOTS = (1, 2, 7, 8)
X_SLOTS = (3, 4, 9, 10)
Y_SLOTS = (0, 5, 6, 11)
MESH = pl.DeviceIdType.MESH
DIRS = ((-1, 0), (1, 0), (0, -1), (0, 1), (-1, -1), (-1, 1), (1, -1), (1, 1))
OPP = (1, 0, 3, 2, 7, 6, 5, 4)
LAYER = NA * 32
ENDS = D * LAYER
EXTRA = ENDS + 2 * NA * 4
FACE = EXTRA + 64
CORNER_ROWS = ((0, 4), (4, 3), (7, 2), (9, 1))
CORNER = NA * 10
EDGE = D * 4 * 16


def profile_of(position, extent):
    width = jnp.float32(PML)
    depth = jnp.maximum(
        jnp.maximum((width - position) / width, (position - (extent - width)) / width), 0.0
    )
    cube = depth * depth * depth
    sigma = sigma_peak * cube
    kappa = 1.0 + (kappa_peak - 1.0) * cube
    alpha = alpha_peak * (1.0 - depth)
    b = jnp.exp(-(sigma / kappa + alpha) * time_step)
    a = sigma * (b - 1.0) / (kappa * (sigma + kappa * alpha))
    inside = depth > 0.0
    return jnp.where(inside, b, 0.0), jnp.where(inside, a, 0.0), 1.0 / kappa


def views(nx, ny):
    gx, gy = lax.axis_index("gx"), lax.axis_index("gy")
    x_first, x_last = gx == 0, gx == nx - 1
    y_first, y_last = gy == 0, gy == ny - 1
    tile = lambda ref: ref.reshape(XR, YP, 128).at[pl.ds(XO, 32), pl.ds(YO, 32), :]
    pxview = lambda ref: ref.reshape(PXR, YP, 128).at[pl.ds(4, 16), pl.ds(YO, 32), :]
    pyrows = lambda ref: ref.reshape(XR, PYP, 128).at[pl.ds(XO, 32), pl.ds(4, 16), :]
    x_layer = jnp.where(x_first, 0, 16)
    y_layer = pl.multiple_of(jnp.where(y_first, 0, 16), 8)
    return x_first, x_last, y_first, y_last, tile, pxview, pyrows, x_layer, y_layer


def store_kernel(nx, ny, *refs):
    refs = list(refs)
    take = lambda n: [refs.pop(0) for _ in range(n)]
    E, H, PZ, PX, PY = take(3), take(3), take(4), take(4), take(4)
    e_out, h_out, psi_out, ZB, sem, edge_sem = refs
    x_first, x_last, y_first, y_last, tile, pxview, pyrows, x_layer, y_layer = views(nx, ny)
    start = lambda copy: copy.start()
    wait = lambda copy: copy.wait()
    stores = [(tile(E[c]), e_out.at[c]) for c in range(3)]
    stores += [(tile(H[c]), h_out.at[c]) for c in range(3)]
    stores += [(tile(PZ[k]), psi_out.at[s]) for k, s in enumerate(Z_SLOTS)]
    stores = [pltpu.make_async_copy(a, b, sem.at[i]) for i, (a, b) in enumerate(stores)]
    for copy in stores:
        copy.start()

    def clear(i, c):
        for k in range(8):
            ZB[pl.ds(pl.multiple_of(i * 64 + k * 8, 8), 8), :] = jnp.zeros((8, 128), jnp.float32)
        return c

    lax.fori_loop(0, 16, clear, 0)
    zb = ZB.reshape(32, 32, 128)
    x_rest = 16 - x_layer
    y_rest = pl.multiple_of(16 - y_layer, 8)

    def rest(act):
        for edge, slots, refs, first in (
            (jnp.logical_or(x_first, x_last), X_SLOTS, PX, 0),
            (jnp.logical_or(y_first, y_last), Y_SLOTS, PY, 4),
        ):

            @pl.when(edge)
            def _(slots=slots, refs=refs, first=first):
                for k, s in enumerate(slots):
                    if first == 0:
                        out = psi_out.at[s, pl.ds(x_layer, 16)]
                        other = psi_out.at[s, pl.ds(x_rest, 16)]
                        kept, none = pxview(refs[k]), zb.at[pl.ds(0, 16)]
                    else:
                        out = psi_out.at[s, :, pl.ds(y_layer, 16)]
                        other = psi_out.at[s, :, pl.ds(y_rest, 16)]
                        kept, none = pyrows(refs[k]), zb.at[:, pl.ds(0, 16)]
                    act(pltpu.make_async_copy(kept, out, edge_sem.at[0, first + k]))
                    act(pltpu.make_async_copy(none, other, edge_sem.at[1, first + k]))

            @pl.when(jnp.logical_not(edge))
            def _(slots=slots, first=first):
                for k, s in enumerate(slots):
                    act(pltpu.make_async_copy(zb, psi_out.at[s], edge_sem.at[0, first + k]))

    rest(start)
    rest(wait)
    for copy in stores:
        copy.wait()


def kernel(nx, ny, e_in, h_in, psi_in, mat_in, eps_in, sig_in, *scratch):
    scratch = list(scratch)
    take = lambda n: [scratch.pop(0) for _ in range(n)]
    E, H, PZ, PX, PY = take(3), take(3), take(4), take(4), take(4)
    KP, DR, MF, MI = take(4)
    xtab, ytab, ztab = take(1)[0], take(1)[0], take(1)[0]
    send_f, recv_f = take(4), take(4)
    send_c, recv_c = take(4), take(4)
    send_e, recv_e = take(4), take(4)
    send_m, recv_m = take(4), take(4)
    send_mc, recv_mc = take(4), take(4)
    in_sem, s_sem, r_sem, sm_sem, rm_sem = take(5)

    gx, gy = lax.axis_index("gx"), lax.axis_index("gy")
    zero = jnp.minimum(gx, 0)
    x_first, x_last, y_first, y_last, tile, pxview, pyrows, x_layer, y_layer = views(nx, ny)
    x_edge = jnp.logical_or(x_first, x_last)
    y_edge = jnp.logical_or(y_first, y_last)
    exists = []
    for dx, dy in DIRS:
        ok = None
        for delta, first, last in ((dx, x_first, x_last), (dy, y_first, y_last)):
            if delta:
                here = jnp.logical_not(first if delta < 0 else last)
                ok = here if ok is None else jnp.logical_and(ok, here)
        exists.append(ok)
    pxbase = jnp.where(x_first, 0, 16)
    pybase = jnp.where(y_first, -4, 12)

    loads = [(h_in.at[c], tile(H[c])) for c in range(3)]
    loads += [(e_in.at[c], tile(E[c])) for c in range(3)]
    loads += [(psi_in.at[s], tile(PZ[k])) for k, s in enumerate(Z_SLOTS)]
    loads += [(mat_in, MI)]
    loads = [pltpu.make_async_copy(a, b, in_sem.at[i]) for i, (a, b) in enumerate(loads)]
    for copy in loads:
        copy.start()
    xloads = [
        pltpu.make_async_copy(
            psi_in.at[s, pl.ds(x_layer, 16)], pxview(PX[k]), in_sem.at[12 + k]
        )
        for k, s in enumerate(X_SLOTS)
    ]
    yloads = [
        pltpu.make_async_copy(
            psi_in.at[s, :, pl.ds(y_layer, 16)], pyrows(PY[k]), in_sem.at[16 + k]
        )
        for k, s in enumerate(Y_SLOTS)
    ]

    @pl.when(x_edge)
    def _():
        for copy in xloads:
            copy.start()

    @pl.when(y_edge)
    def _():
        for copy in yloads:
            copy.start()

    barrier = pltpu.get_barrier_semaphore()
    count = 0
    for d, (dx, dy) in enumerate(DIRS):
        count = count + exists[d].astype(jnp.int32)

        @pl.when(exists[d])
        def _(dx=dx, dy=dy):
            pl.semaphore_signal(barrier, inc=1, device_id=(gx + dx, gy + dy), device_id_type=MESH)

    row = lax.broadcasted_iota(jnp.int32, (8, 128), 0)
    lane = lax.broadcasted_iota(jnp.int32, (8, 128), 1)
    zeros = jnp.zeros((8, 128), jnp.float32)
    for half, shift in ((0, 0.5), (1, 0.0)):
        for k, value in enumerate(profile_of(lane.astype(jnp.float32) + shift, 128)):
            ztab[(half * 3 + k) * 8 : (half * 3 + k) * 8 + 8, :] = value
        for i in range(6):
            for tab, offset, extent in (
                (xtab, gx * 32 - XO, nx * 32),
                (ytab, gy * 32 - YO, ny * 32),
            ):
                position = (row + (i * 8 + offset)).astype(jnp.float32) + shift
                for k, value in enumerate(profile_of(position, extent)):
                    at = (half * 3 + k) * 48 + i * 8
                    tab[at : at + 8, :] = value

    for ref in E + H:
        for x in (0, 1, 2, 3, 4, 37, 38, 39, 40, 41):
            for k in range(6):
                ref[x * YP + k * 8 : x * YP + k * 8 + 8, :] = zeros

    def clear_rim(i, c):
        base = pl.multiple_of((i + XO) * YP, 8)
        for ref in E + H:
            ref[pl.ds(base, 8), :] = zeros
            ref[pl.ds(base + 40, 8), :] = zeros
        return c

    lax.fori_loop(0, 32, clear_rim, 0)

    def clear_beside(i, c):
        for ref in PX:
            for start in (0, 20 * YP):
                ref[pl.ds(pl.multiple_of(start + i * 8, 8), 8), :] = zeros
        return c

    lax.fori_loop(0, 4 * YP // 8, clear_beside, 0)

    for copy in loads:
        copy.wait()

    @pl.when(x_edge)
    def _():
        for copy in xloads:
            copy.wait()

    @pl.when(y_edge)
    def _():
        for copy in yloads:
            copy.wait()

    keep_of, drive_of = [], []
    for n in range(NMAT):
        eps = jnp.full((8, 128), eps_in[n], jnp.float32)
        loss = jnp.full((8, 128), sig_in[n], jnp.float32) * time_step / (2.0 * eps)
        keep_of.append((1.0 - loss) / (1.0 + loss))
        drive_of.append((time_step / eps) / (1.0 + loss))

    def choose(bits, table):
        for bit in bits:
            table = [jnp.where(bit, table[i + 1], table[i]) for i in range(0, len(table), 2)]
        return table[0]

    def coefficients(base):
        number = MF[pl.ds(base, 8), :].astype(jnp.int32)
        bits = [(number & (1 << k)) != 0 for k in range(3)]
        KP[pl.ds(base, 8), :] = choose(bits, keep_of)
        DR[pl.ds(base, 8), :] = choose(bits, drive_of)

    at = lambda x, y: (x + XO) * YP + YO + y

    def own_material(x, c):
        for k in range(4):
            MF[pl.ds(at(x, 8 * k), 8), :] = MI[
                pl.ds(pl.multiple_of(x * 32 + 8 * k, 8), 8), :
            ].astype(jnp.float32)
            coefficients(at(x, 8 * k))
        return c

    lax.fori_loop(0, 32, own_material, 0)
    pl.semaphore_wait(barrier, count)

    def remote(d, src, dst, ssem, rsem):
        dx, dy = DIRS[d]
        return pltpu.make_async_remote_copy(
            src_ref=src,
            dst_ref=dst,
            send_sem=ssem,
            recv_sem=rsem,
            device_id=(gx + dx, gy + dy),
            device_id_type=MESH,
        )

    def guarded(d, *copies):
        @pl.when(exists[d])
        def _():
            for copy in copies:
                copy.start()

    def layer_rows(d, layer, q, low):
        if low is None:
            place = layer if DIRS[d][d // 2] < 0 else 31 - layer
        else:
            place = -1 - layer if DIRS[d][d // 2] < 0 else 32 + layer
        if d < 2:
            return pl.ds(at(place, 8 * q) + zero, 8)
        return pl.ds(at(8 * q, place) + zero, 8, stride=YP)

    def pack(parts):
        lanes = lax.broadcasted_iota(jnp.int32, parts[0].shape, 1)
        out = pltpu.roll(parts[3], 112, 1)
        for s in (2, 1, 0):
            out = jnp.where(lanes < 32 * (s + 1), pltpu.roll(parts[s], 32 * s + 16, 1), out)
        return out

    def gather(rows):
        return [ref[rows, :] for ref in E + H] + [pack([ref[rows, :] for ref in PZ])]

    def scatter(rows, values):
        for ref, value in zip(E + H, values):
            ref[rows, :] = value
        for s, ref in enumerate(PZ):
            ref[rows, :] = pltpu.roll(values[6], 112 - 32 * s, 1)

    def end_rows(d, layer, end, low):
        if low is None:
            place = layer if DIRS[d][d // 2] < 0 else 31 - layer
        else:
            place = -1 - layer if DIRS[d][d // 2] < 0 else 32 + layer
        if d < 2:
            return pl.ds(at(place, 30 * end) + zero, 2)
        return pl.ds(at(30 * end, place) + zero, 2, stride=YP)

    def face_copy(d, blk, start, n, k, incoming):
        span = pl.ds(start, n)
        to = d if incoming else OPP[d]
        return remote(
            d, send_f[d].at[span], recv_f[to].at[blk, span], s_sem.at[d, k], r_sem.at[blk, to, k]
        )

    def send_layer(d, layer, blk):
        buf = send_f[d]
        for q in range(4):
            for k, value in enumerate(gather(layer_rows(d, layer, q, None))):
                buf[pl.ds(pl.multiple_of(layer * LAYER + k * 32 + q * 8, 8), 8), :] = value
        guarded(d, face_copy(d, blk, pl.multiple_of(layer * LAYER, 8), LAYER, layer, False))

    extra_fields = {1: (H[1], H[2]), 3: (H[2], H[0])}
    tail_rows = lambda d: (FACE if d in (1, 3) else EXTRA) - ENDS

    def send_tail(d, blk):
        buf = send_f[d]
        for layer in range(2):
            for end in range(2):
                for k, value in enumerate(gather(end_rows(d, D + layer, end, None))):
                    s = ENDS + layer * NA * 4 + k * 4 + end * 2
                    buf[s : s + 2, :] = value
        if d in extra_fields:
            for k, ref in enumerate(extra_fields[d]):
                for q in range(4):
                    s = EXTRA + k * 32 + q * 8
                    buf[s : s + 8, :] = ref[layer_rows(d, D, q, None), :]
        guarded(d, face_copy(d, blk, ENDS, tail_rows(d), D, False))

    def send_corner(d, blk):
        buf, (dx, dy) = send_c[d - 4], DIRS[d]
        for i, (first, n) in enumerate(CORNER_ROWS):
            x = i if dx < 0 else 31 - i
            rows = pl.ds(at(x, 0 if dy < 0 else 32 - n) + zero, n)
            for k, value in enumerate(gather(rows)):
                buf[k * 10 + first : k * 10 + first + n, :] = value
        copy = remote(
            d, buf, recv_c[OPP[d] - 4].at[blk], s_sem.at[d, 0], r_sem.at[blk, OPP[d], 0]
        )
        guarded(d, copy)

    def edge_rows(d, layer, low):
        if low is None:
            place = layer if DIRS[d][d // 2] < 0 else 31 - layer
        else:
            place = -1 - layer if DIRS[d][d // 2] < 0 else 32 + layer
        if d < 2:
            return [pl.ds((place + XO) * PYP + 4 + 8 * q + zero, 8) for q in range(2)]
        return [pl.ds((8 * q + 4) * YP + YO + place + zero, 8, stride=YP) for q in range(2)]

    def send_edge(d, blk):
        @pl.when(jnp.logical_and(exists[d], y_edge if d < 2 else x_edge))
        def _():
            buf = send_e[d]
            for layer in range(D):
                for k, ref in enumerate(PY if d < 2 else PX):
                    for q, rows in enumerate(edge_rows(d, layer, None)):
                        s = layer * 64 + k * 16 + q * 8
                        buf[s : s + 8, :] = ref[rows, :]
            remote(
                d, buf, recv_e[OPP[d]].at[blk], s_sem.at[d, D + 1], r_sem.at[blk, OPP[d], D + 1]
            ).start()

    def receive_face(d, blk):
        @pl.when(exists[d])
        def _():
            buf = recv_f[d]
            for k in range(D + 1):
                start, size = (k * LAYER, LAYER) if k < D else (ENDS, tail_rows(d))
                face_copy(d, blk, start, size, k, True).wait_send()
                if k == D:
                    size = tail_rows(OPP[d])
                face_copy(d, blk, start, size, k, True).wait_recv()

            def unpack(layer, c):
                for q in range(4):
                    scatter(
                        layer_rows(d, layer, q, True),
                        [
                            buf[blk, pl.ds(pl.multiple_of(layer * LAYER + k * 32 + q * 8, 8), 8), :]
                            for k in range(NA)
                        ],
                    )
                return c

            lax.fori_loop(0, D, unpack, 0)
            for layer in range(2):
                for end in range(2):
                    s = ENDS + layer * NA * 4 + end * 2
                    scatter(
                        end_rows(d, D + layer, end, True),
                        [buf[blk, s + 4 * k : s + 4 * k + 2, :] for k in range(NA)],
                    )
            if OPP[d] in extra_fields:
                for k, ref in enumerate(extra_fields[OPP[d]]):
                    for q in range(4):
                        s = EXTRA + k * 32 + q * 8
                        ref[layer_rows(d, D, q, True), :] = buf[blk, s : s + 8, :]

    def receive_corner(d, blk):
        @pl.when(exists[d])
        def _():
            buf, (dx, dy) = recv_c[d - 4], DIRS[d]
            copy = remote(d, send_c[d - 4], buf.at[blk], s_sem.at[d, 0], r_sem.at[blk, d, 0])
            copy.wait_recv()
            copy.wait_send()
            for i, (first, n) in enumerate(CORNER_ROWS):
                x = -1 - i if dx < 0 else 32 + i
                s = lambda k: k * 10 + first
                scatter(
                    pl.ds(at(x, -n if dy < 0 else 32) + zero, n),
                    [buf[blk, s(k) : s(k) + n, :] for k in range(NA)],
                )

    def receive_edge(d, blk):
        @pl.when(jnp.logical_and(exists[d], y_edge if d < 2 else x_edge))
        def _():
            buf = recv_e[d]
            copy = remote(d, send_e[d], buf.at[blk], s_sem.at[d, D + 1], r_sem.at[blk, d, D + 1])
            copy.wait_recv()
            copy.wait_send()
            for layer in range(D):
                for k, ref in enumerate(PY if d < 2 else PX):
                    for q, rows in enumerate(edge_rows(d, layer, True)):
                        s = layer * 64 + k * 16 + q * 8
                        ref[rows, :] = buf[blk, s : s + 8, :]

    for d in range(4):
        for layer in range(M):
            for q in range(4):
                s = layer * 32 + q * 8
                send_m[d][s : s + 8, :] = MF[layer_rows(d, layer, q, None), :]
        guarded(d, remote(d, send_m[d], recv_m[OPP[d]], sm_sem.at[d], rm_sem.at[OPP[d]]))
    for d in range(4, 8):
        dx, dy = DIRS[d]
        for i in range(M):
            rows = pl.ds(at(i if dx < 0 else 31 - i, 0 if dy < 0 else 28) + zero, 4)
            send_mc[d - 4][i * 4 : i * 4 + 4, :] = MF[rows, :]
        guarded(
            d, remote(d, send_mc[d - 4], recv_mc[OPP[d] - 4], sm_sem.at[d], rm_sem.at[OPP[d]])
        )

    def receive_material():
        for x in (0, 1, 2, 3, 4, 37, 38, 39, 40, 41):
            for k in range(6):
                MF[x * YP + k * 8 : x * YP + k * 8 + 8, :] = zeros

        def clear_side(x, c):
            MF[pl.ds(pl.multiple_of((x + XO) * YP, 8), 8), :] = zeros
            MF[pl.ds(pl.multiple_of((x + XO) * YP + 40, 8), 8), :] = zeros
            return c

        lax.fori_loop(0, 32, clear_side, 0)
        for d in range(8):

            @pl.when(exists[d])
            def _(d=d):
                dx, dy = DIRS[d]
                if d < 4:
                    copy = remote(d, send_m[d], recv_m[d], sm_sem.at[d], rm_sem.at[d])
                else:
                    copy = remote(d, send_mc[d - 4], recv_mc[d - 4], sm_sem.at[d], rm_sem.at[d])
                copy.wait_recv()
                copy.wait_send()
                for i in range(M):
                    if d < 4:
                        for q in range(4):
                            s = i * 32 + q * 8
                            MF[layer_rows(d, i, q, True), :] = recv_m[d][s : s + 8, :]
                    else:
                        x = -1 - i if dx < 0 else 32 + i
                        rows = pl.ds(at(x, -4 if dy < 0 else 32) + zero, 4)
                        MF[rows, :] = recv_mc[d - 4][i * 4 : i * 4 + 4, :]

        def whole_row(x, c):
            for k in range(5):
                coefficients(at(x, 8 * k - 4) + zero)
            return c

        def ends_of_row(x, c):
            for k in (0, 4):
                coefficients(at(x, 8 * k - 4) + zero)
            return c

        lax.fori_loop(-4, 0, whole_row, 0)
        lax.fori_loop(32, 36, whole_row, 0)
        lax.fori_loop(0, 32, ends_of_row, 0)

    def table(tab, half, k, start, n):
        return tab[pl.ds(half * 3 * n + k * n + start, 8), :]

    def half_step(half, x0, starts, mask_of, px, py):
        source, target = (E, H) if half == 0 else (H, E)
        step = 1 if half == 0 else -1
        zc = [ztab[(half * 3 + k) * 8 : (half * 3 + k) * 8 + 8, :] for k in range(3)]
        keep_lane = lane < 127 if half == 0 else lane > 0
        for r in range(U):
            x = x0 + r
            if px:
                xc = [
                    jnp.broadcast_to(xtab[pl.ds((half * 3 + k) * 48 + x + XO, 1), :], (8, 128))
                    for k in range(3)
                ]
            for i, y in enumerate(starts):
                rows = lambda dx, dy: pl.ds(at(x + dx, y + dy) + zero, 8)
                here = rows(0, 0)
                mask = mask_of(r, x, i)

                def put(ref, where, value):
                    pltpu.store(ref.at[where, :], value, mask=mask)

                def diff(a, b):
                    return a - b if half == 0 else b - a

                s0, s1, s2 = (ref[here, :] for ref in source)
                sh = 127 if half == 0 else 1
                turn = lambda v: jnp.where(keep_lane, pltpu.roll(v, sh, 1), 0.0)
                dz1, dz0 = diff(turn(s1), s1), diff(turn(s0), s0)
                dy2 = diff(source[2][rows(0, step), :], s2)
                dy0 = diff(source[0][rows(0, step), :], s0)
                dx2 = diff(source[2][rows(step, 0), :], s2)
                dx1 = diff(source[1][rows(step, 0), :], s1)

                def term(d, coef, ref, where):
                    b, a, q = coef
                    new = b * ref[where, :] + a * d
                    put(ref, where, new)
                    return q * d + new

                tz1 = term(dz1, zc, PZ[2 * half], here)
                tz0 = term(dz0, zc, PZ[2 * half + 1], here)
                if px:
                    there = pl.ds((x - pxbase + 4) * YP + YO + y + zero, 8)
                    tx2 = term(dx2, xc, PX[2 * half], there)
                    tx1 = term(dx1, xc, PX[2 * half + 1], there)
                else:
                    tx2, tx1 = dx2, dx1
                if i in py:
                    yc = [
                        ytab[pl.ds((half * 3 + k) * 48 + YO + y + zero, 8), :] for k in range(3)
                    ]
                    there = pl.ds((x + XO) * PYP + (y - py[i]) + zero, 8)
                    ty2 = term(dy2, yc, PY[2 * half], there)
                    ty0 = term(dy0, yc, PY[2 * half + 1], there)
                else:
                    ty2, ty0 = dy2, dy0
                curls = (ty2 - tz1, tz0 - tx2, tx1 - ty0)
                if half == 0:
                    for ref, c in zip(target, curls):
                        put(ref, here, ref[here, :] - time_step * c)
                else:
                    kp, dr = KP[here, :], DR[here, :]
                    for ref, c in zip(target, curls):
                        put(ref, here, kp * ref[here, :] + dr * c)

    px0 = jnp.where(x_first, 0, jnp.where(x_last, 16, -32))
    px1 = jnp.where(x_edge, px0 + 16, -32)

    def groups(half, xs, xe, starts, mask_of, py):
        n = (xe - xs + U - 1) // U
        ia = jnp.clip((px0 - xs + 64) // U - 64 // U, 0, n)
        ib = jnp.clip((px1 - xs + 64 + U - 1) // U - 64 // U, 0, n)

        def plain(part, c):
            def one(i, c):
                half_step(half, xs + U * i, starts, mask_of, False, py)
                return c

            return lax.fori_loop(jnp.where(part == 0, 0, ib), jnp.where(part == 0, ia, n), one, c)

        lax.fori_loop(0, 2, plain, 0)

        def layered(i, c):
            half_step(half, xs + U * i, starts, mask_of, True, py)
            return c

        lax.fori_loop(ia, ib, layered, 0)

    def by_place(run, low, high):
        @pl.when(y_first)
        def _():
            run({i: -4 for i in low})

        @pl.when(y_last)
        def _():
            run({i: 12 for i in high})

        @pl.when(jnp.logical_not(y_edge))
        def _():
            run({})

    def inner_range(t, half, first, last):
        lo = jnp.where(first, 0, t - 1 + half)
        hi = jnp.where(last, 32, 32 - t)
        return lo, hi

    def within(v, lo, hi):
        return jnp.logical_and(v >= lo, v < hi)

    starts_a = (0, 8, 16, 24)
    starts_b = (-4, 4, 12, 20, 28)

    def pass_a(t, py):
        for half in range(2):
            xlo, xhi = inner_range(t, half, x_first, x_last)
            ylo, yhi = inner_range(t, half, y_first, y_last)

            def mask_of(r, x, i, xlo=xlo, xhi=xhi, ylo=ylo, yhi=yhi):
                ok = within(x, xlo, xhi).astype(jnp.int32)
                if i in (0, 3):
                    return within(row + starts_a[i], ylo, jnp.where(ok > 0, yhi, -99))
                return row >= 8 - 8 * ok

            groups(half, xlo, xhi, starts_a, mask_of, py)

    def pass_b(t, py):
        ya = jnp.where(y_first, 0, -99)
        yb = jnp.where(y_last, 32, 99)
        for half in range(2):
            xc, xd = inner_range(t, half, x_first, x_last)
            yc, yd = inner_range(t, half, y_first, y_last)
            grow = t - 1 + half
            xa = jnp.where(x_first, 0, -t)
            xb = jnp.where(x_last, 32, 32 + grow)
            wa = jnp.where(y_first, 0, -t)
            wb = jnp.where(y_last, 32, 32 + grow)
            low = jnp.maximum(-t, t - 5 + half)
            high = 32 - t
            xs = jnp.where(x_first, 0, low + U)
            xe = jnp.where(x_last, 32, high)

            def mask_of(r, x, i, xa=xa, xb=xb, xc=xc, xd=xd, yc=yc, yd=yd, wa=wa, wb=wb):
                border = jnp.logical_or(within(x, xa, xc), within(x, xd, xb))
                if i not in (0, 4):
                    return row >= 8 - 8 * border.astype(jnp.int32)
                y = row + starts_b[i]
                if i == 0:
                    return within(y, jnp.where(border, ya, wa), jnp.where(border, 99, yc))
                return within(y, jnp.where(border, -99, yd), jnp.where(border, yb, wb))

            def ends_mask(r, x, i, yc=yc, yd=yd, wa=wa, wb=wb, xe=xe):
                y = row + (-4 if i == 0 else 28)
                if i == 0:
                    return within(y, wa, jnp.where(x < xe, yc, -99))
                return within(y, yd, jnp.where(x < xe, wb, -99))

            def border(p, c, half=half, low=low, high=high, mask_of=mask_of):
                half_step(half, jnp.where(p == 0, low, high), starts_b, mask_of, False, py)
                return c

            lax.fori_loop(jnp.where(x_first, 1, 0), jnp.where(x_last, 1, 2), border, 0)
            ends_py = {k // 4: v for k, v in py.items() if k in (0, 4)}
            groups(half, xs, xe, (-4, 28), ends_mask, ends_py)

            def outside_mask(r, x, i, low=low, yc=yc, yd=yd, wa=wa, wb=wb):
                y = row + (-4 if i == 0 else 28)
                if i == 0:
                    return within(y, wa, jnp.where(x < low, yc, -99))
                return within(y, yd, jnp.where(x < low, wb, -99))

            @pl.when(jnp.logical_and(jnp.logical_not(x_first), low + 5 - t - half > 0))
            def _(half=half, outside_mask=outside_mask):
                half_step(half, t - 5 + half, (-4, 28), outside_mask, False, ends_py)

    def block(turn, c):
        blk = turn % 2

        def step_a(t, c):
            @pl.when(t <= D)
            def _():
                send_layer(1, t - 1, blk)
                send_layer(3, t - 1, blk)

            by_place(lambda py: pass_a(t, py), (0, 1), (2, 3))

            @pl.when(t <= D)
            def _():
                send_layer(0, t - 1, blk)
                send_layer(2, t - 1, blk)

            @pl.when(t == D)
            def _():
                for d in range(4):
                    send_tail(d, blk)
                for d in range(4, 8):
                    send_corner(d, blk)
                for d in range(4):
                    send_edge(d, blk)

            return c

        lax.fori_loop(1, M + 1, step_a, 0)

        @pl.when(turn == 0)
        def _():
            receive_material()

        for d in range(4, 8):
            receive_corner(d, blk)
        for d in range(4):
            receive_edge(d, blk)
        for d in (2, 3, 0, 1):
            receive_face(d, blk)

        def step_b(t, c):
            by_place(lambda py: pass_b(t, py), (0, 1, 2), (2, 3, 4))
            return c

        lax.fori_loop(1, M + 1, step_b, 0)
        return c

    lax.fori_loop(0, STEPS // M, block, 0)


def solution(mesh):
    nx, ny = mesh.shape["gx"], mesh.shape["gy"]
    f32 = jnp.float32
    field = P(None, "gx", "gy", None)

    def shards(e_field, h_field, psi, material, eps_table, sigma_table):
        big = pltpu.VMEM((XR * YP, 128), f32)
        dma = pltpu.SemaphoreType.DMA
        kept = [(XR * YP, 128)] * 10 + [(PXR * YP, 128)] * 4 + [(XR * PYP, 128)] * 4
        scratch = [big, big, big, pltpu.VMEM((1024, 128), jnp.int32)]
        scratch += [pltpu.VMEM((6 * 48, 128), f32)] * 2 + [pltpu.VMEM((48, 128), f32)]
        scratch += [pltpu.VMEM((FACE, 128), f32)] * 4 + [pltpu.VMEM((2, FACE, 128), f32)] * 4
        scratch += [pltpu.VMEM((CORNER, 128), f32)] * 4 + [pltpu.VMEM((2, CORNER, 128), f32)] * 4
        scratch += [pltpu.VMEM((EDGE, 128), f32)] * 4 + [pltpu.VMEM((2, EDGE, 128), f32)] * 4
        scratch += [pltpu.VMEM((128, 128), f32)] * 8 + [pltpu.VMEM((16, 128), f32)] * 8
        scratch += [
            dma((20,)),
            dma((8, D + 2)),
            dma((2, 8, D + 2)),
            dma((8,)),
            dma((8,)),
        ]
        anywhere = pl.BlockSpec(memory_space=pl.ANY)
        smem = pl.BlockSpec(memory_space=pltpu.SMEM)
        vmem = pl.BlockSpec(memory_space=pltpu.VMEM)
        state = pl.pallas_call(
            functools.partial(kernel, nx, ny),
            out_shape=[pltpu.VMEM(shape, f32) for shape in kept],
            in_specs=[anywhere] * 4 + [smem] * 2,
            out_specs=[vmem] * len(kept),
            scratch_shapes=scratch,
            compiler_params=pltpu.CompilerParams(
                collective_id=0, has_side_effects=True, vmem_limit_bytes=40 << 20
            ),
        )(e_field, h_field, psi, material.reshape(1024, 128), eps_table, sigma_table)
        state = [pltpu.with_memory_space_constraint(a, pltpu.VMEM) for a in state]
        return pl.pallas_call(
            functools.partial(store_kernel, nx, ny),
            out_shape=[jax.ShapeDtypeStruct(a.shape, f32) for a in (e_field, h_field, psi)],
            in_specs=[vmem] * len(kept),
            out_specs=[anywhere] * 3,
            scratch_shapes=[pltpu.VMEM((1024, 128), f32), dma((10,)), dma((2, 8))],
            compiler_params=pltpu.CompilerParams(vmem_limit_bytes=8 << 20),
        )(*state)

    return jax.shard_map(
        shards,
        mesh=mesh,
        in_specs=(field, field, field, P("gx", "gy", None), P(), P()),
        out_specs=(field, field, field),
        check_vma=False,
    )
```

```python
import functools

import jax
import jax.numpy as jnp
from jax import lax
from jax.experimental import pallas as pl
from jax.experimental.pallas import tpu as pltpu
from jax.sharding import PartitionSpec as P

PML = 16
STEPS = 16
NMAT = 8
time_step = 0.5
sigma_peak = 3.0
kappa_peak = 5.0
alpha_peak = 0.05

M = 4
D = 2
PXR = 32
PXO = 8
XO, XR = 5, 42
YO, YP = 8, 48
PYP = 24
U, UA, UE = 4, 4, 8
NA = 7
Z_SLOTS = (1, 2, 7, 8)
X_SLOTS = (3, 4, 9, 10)
Y_SLOTS = (0, 5, 6, 11)
MESH = pl.DeviceIdType.MESH
DIRS = ((-1, 0), (1, 0), (0, -1), (0, 1), (-1, -1), (-1, 1), (1, -1), (1, 1))
OPP = (1, 0, 3, 2, 7, 6, 5, 4)
LAYER = NA * 32
ENDS = D * LAYER
EXTRA = ENDS + 2 * NA * 4
FACE = EXTRA + 64
CORNER_ROWS = ((0, 4), (4, 2), (6, 1), (7, 1))
CORNER = NA * 8
EDGE = D * 4 * 16


def profile_of(position, extent):
    width = jnp.float32(PML)
    depth = jnp.maximum(
        jnp.maximum((width - position) / width, (position - (extent - width)) / width), 0.0
    )
    cube = depth * depth * depth
    sigma = sigma_peak * cube
    kappa = 1.0 + (kappa_peak - 1.0) * cube
    alpha = alpha_peak * (1.0 - depth)
    b = jnp.exp(-(sigma / kappa + alpha) * time_step)
    a = sigma * (b - 1.0) / (kappa * (sigma + kappa * alpha))
    inside = depth > 0.0
    return jnp.where(inside, b, 0.0), jnp.where(inside, a, 0.0), 1.0 / kappa


def views(nx, ny):
    gx, gy = lax.axis_index("gx"), lax.axis_index("gy")
    x_first, x_last = gx == 0, gx == nx - 1
    y_first, y_last = gy == 0, gy == ny - 1
    tile = lambda ref: ref.reshape(XR, YP, 128).at[pl.ds(XO, 32), pl.ds(YO, 32), :]
    pxview = lambda ref: ref.reshape(PXR, YP, 128).at[pl.ds(PXO, 16), pl.ds(YO, 32), :]
    pyrows = lambda ref: ref.reshape(XR, PYP, 128).at[pl.ds(XO, 32), pl.ds(4, 16), :]
    x_layer = jnp.where(x_first, 0, 16)
    y_layer = pl.multiple_of(jnp.where(y_first, 0, 16), 8)
    return x_first, x_last, y_first, y_last, tile, pxview, pyrows, x_layer, y_layer


def store_kernel(nx, ny, *refs):
    refs = list(refs)
    take = lambda n: [refs.pop(0) for _ in range(n)]
    E, H, PZ, PX, PY = take(3), take(3), take(4), take(4), take(4)
    e_out, h_out, psi_out, ZB, sem, edge_sem = refs
    x_first, x_last, y_first, y_last, tile, pxview, pyrows, x_layer, y_layer = views(nx, ny)
    start = lambda copy: copy.start()
    wait = lambda copy: copy.wait()
    stores = [(tile(E[c]), e_out.at[c]) for c in range(3)]
    stores += [(tile(H[c]), h_out.at[c]) for c in range(3)]
    stores += [(tile(PZ[k]), psi_out.at[s]) for k, s in enumerate(Z_SLOTS)]
    stores = [pltpu.make_async_copy(a, b, sem.at[i]) for i, (a, b) in enumerate(stores)]
    for copy in stores:
        copy.start()

    def clear(i, c):
        for k in range(8):
            ZB[pl.ds(pl.multiple_of(i * 64 + k * 8, 8), 8), :] = jnp.zeros((8, 128), jnp.float32)
        return c

    lax.fori_loop(0, 16, clear, 0)
    zb = ZB.reshape(32, 32, 128)
    x_rest = 16 - x_layer
    y_rest = pl.multiple_of(16 - y_layer, 8)

    def rest(act):
        for edge, slots, refs, first in (
            (jnp.logical_or(x_first, x_last), X_SLOTS, PX, 0),
            (jnp.logical_or(y_first, y_last), Y_SLOTS, PY, 4),
        ):

            @pl.when(edge)
            def _(slots=slots, refs=refs, first=first):
                for k, s in enumerate(slots):
                    if first == 0:
                        out = psi_out.at[s, pl.ds(x_layer, 16)]
                        other = psi_out.at[s, pl.ds(x_rest, 16)]
                        kept, none = pxview(refs[k]), zb.at[pl.ds(0, 16)]
                    else:
                        out = psi_out.at[s, :, pl.ds(y_layer, 16)]
                        other = psi_out.at[s, :, pl.ds(y_rest, 16)]
                        kept, none = pyrows(refs[k]), zb.at[:, pl.ds(0, 16)]
                    act(pltpu.make_async_copy(kept, out, edge_sem.at[0, first + k]))
                    act(pltpu.make_async_copy(none, other, edge_sem.at[1, first + k]))

            @pl.when(jnp.logical_not(edge))
            def _(slots=slots, first=first):
                for k, s in enumerate(slots):
                    act(pltpu.make_async_copy(zb, psi_out.at[s], edge_sem.at[0, first + k]))

    rest(start)
    rest(wait)
    for copy in stores:
        copy.wait()


def kernel(nx, ny, e_in, h_in, psi_in, mat_in, eps_in, sig_in, *scratch):
    scratch = list(scratch)
    take = lambda n: [scratch.pop(0) for _ in range(n)]
    E, H, PZ, PX, PY = take(3), take(3), take(4), take(4), take(4)
    KP, DR, MF, MI = take(4)
    xtab, ytab, ztab = take(1)[0], take(1)[0], take(1)[0]
    send_f, recv_f = take(4), take(4)
    send_c, recv_c = take(4), take(4)
    send_e, recv_e = take(4), take(4)
    send_m, recv_m = take(4), take(4)
    send_mc, recv_mc = take(4), take(4)
    in_sem, s_sem, r_sem, sm_sem, rm_sem = take(5)

    gx, gy = lax.axis_index("gx"), lax.axis_index("gy")
    zero = jnp.minimum(gx, 0)
    x_first, x_last, y_first, y_last, tile, pxview, pyrows, x_layer, y_layer = views(nx, ny)
    x_edge = jnp.logical_or(x_first, x_last)
    y_edge = jnp.logical_or(y_first, y_last)
    exists = []
    for dx, dy in DIRS:
        ok = None
        for delta, first, last in ((dx, x_first, x_last), (dy, y_first, y_last)):
            if delta:
                here = jnp.logical_not(first if delta < 0 else last)
                ok = here if ok is None else jnp.logical_and(ok, here)
        exists.append(ok)
    pxbase = jnp.where(x_first, 0, 16)
    pybase = jnp.where(y_first, -4, 12)

    loads = [(h_in.at[c], tile(H[c])) for c in range(3)]
    loads += [(e_in.at[c], tile(E[c])) for c in range(3)]
    loads += [(psi_in.at[s], tile(PZ[k])) for k, s in enumerate(Z_SLOTS)]
    loads += [(mat_in, MI)]
    loads = [pltpu.make_async_copy(a, b, in_sem.at[i]) for i, (a, b) in enumerate(loads)]
    for copy in loads:
        copy.start()
    xloads = [
        pltpu.make_async_copy(
            psi_in.at[s, pl.ds(x_layer, 16)], pxview(PX[k]), in_sem.at[12 + k]
        )
        for k, s in enumerate(X_SLOTS)
    ]
    yloads = [
        pltpu.make_async_copy(
            psi_in.at[s, :, pl.ds(y_layer, 16)], pyrows(PY[k]), in_sem.at[16 + k]
        )
        for k, s in enumerate(Y_SLOTS)
    ]

    @pl.when(x_edge)
    def _():
        for copy in xloads:
            copy.start()

    @pl.when(y_edge)
    def _():
        for copy in yloads:
            copy.start()

    barrier = pltpu.get_barrier_semaphore()
    count = 0
    for d, (dx, dy) in enumerate(DIRS):
        count = count + exists[d].astype(jnp.int32)

        @pl.when(exists[d])
        def _(dx=dx, dy=dy):
            pl.semaphore_signal(barrier, inc=1, device_id=(gx + dx, gy + dy), device_id_type=MESH)

    row = lax.broadcasted_iota(jnp.int32, (8, 128), 0)
    lane = lax.broadcasted_iota(jnp.int32, (8, 128), 1)
    zeros = jnp.zeros((8, 128), jnp.float32)
    for half, shift in ((0, 0.5), (1, 0.0)):
        for k, value in enumerate(profile_of(lane.astype(jnp.float32) + shift, 128)):
            ztab[(half * 3 + k) * 8 : (half * 3 + k) * 8 + 8, :] = value
        for i in range(6):
            for tab, offset, extent in (
                (xtab, gx * 32 - XO, nx * 32),
                (ytab, gy * 32 - YO, ny * 32),
            ):
                position = (row + (i * 8 + offset)).astype(jnp.float32) + shift
                for k, value in enumerate(profile_of(position, extent)):
                    at = (half * 3 + k) * 48 + i * 8
                    tab[at : at + 8, :] = value

    for ref in E + H:
        for x in (0, 1, 2, 3, 4, 37, 38, 39, 40, 41):
            for k in range(6):
                ref[x * YP + k * 8 : x * YP + k * 8 + 8, :] = zeros

    def clear_rim(i, c):
        base = pl.multiple_of((i + XO) * YP, 8)
        for ref in E + H:
            ref[pl.ds(base, 8), :] = zeros
            ref[pl.ds(base + 40, 8), :] = zeros
        return c

    lax.fori_loop(0, 32, clear_rim, 0)

    def clear_beside(i, c):
        for ref in PX:
            for start in (0, (PXO + 16) * YP):
                ref[pl.ds(pl.multiple_of(start + i * 8, 8), 8), :] = zeros
        return c

    lax.fori_loop(0, PXO * YP // 8, clear_beside, 0)

    for copy in loads:
        copy.wait()

    @pl.when(x_edge)
    def _():
        for copy in xloads:
            copy.wait()

    @pl.when(y_edge)
    def _():
        for copy in yloads:
            copy.wait()

    keep_of, drive_of = [], []
    for n in range(NMAT):
        eps = jnp.full((8, 128), eps_in[n], jnp.float32)
        loss = jnp.full((8, 128), sig_in[n], jnp.float32) * time_step / (2.0 * eps)
        keep_of.append((1.0 - loss) / (1.0 + loss))
        drive_of.append((time_step / eps) / (1.0 + loss))

    def choose(bits, table):
        for bit in bits:
            table = [jnp.where(bit, table[i + 1], table[i]) for i in range(0, len(table), 2)]
        return table[0]

    def coefficients(ref, table, bases):
        for base in bases:
            number = MF[pl.ds(base, 8), :].astype(jnp.int32)
            bits = [(number & (1 << k)) != 0 for k in range(3)]
            ref[pl.ds(base, 8), :] = choose(bits, table)

    def all_coefficients(first, last, ys):
        for ref, table in ((KP, keep_of), (DR, drive_of)):

            def one(x, c, ref=ref, table=table):
                coefficients(ref, table, [at(x, y) + zero for y in ys])
                return c

            lax.fori_loop(first, last, one, 0)

    at = lambda x, y: (x + XO) * YP + YO + y

    def own_material(x, c):
        for k in range(4):
            MF[pl.ds(at(x, 8 * k), 8), :] = MI[
                pl.ds(pl.multiple_of(x * 32 + 8 * k, 8), 8), :
            ].astype(jnp.float32)
        return c

    lax.fori_loop(0, 32, own_material, 0)
    all_coefficients(0, 32, (0, 8, 16, 24))
    pl.semaphore_wait(barrier, count)

    def remote(d, src, dst, ssem, rsem):
        dx, dy = DIRS[d]
        return pltpu.make_async_remote_copy(
            src_ref=src,
            dst_ref=dst,
            send_sem=ssem,
            recv_sem=rsem,
            device_id=(gx + dx, gy + dy),
            device_id_type=MESH,
        )

    def guarded(d, *copies):
        @pl.when(exists[d])
        def _():
            for copy in copies:
                copy.start()

    def layer_rows(d, layer, q, low):
        if low is None:
            place = layer if DIRS[d][d // 2] < 0 else 31 - layer
        else:
            place = -1 - layer if DIRS[d][d // 2] < 0 else 32 + layer
        if d < 2:
            return pl.ds(at(place, 8 * q) + zero, 8)
        return pl.ds(at(8 * q, place) + zero, 8, stride=YP)

    def pack(parts):
        lanes = lax.broadcasted_iota(jnp.int32, parts[0].shape, 1)
        out = pltpu.roll(parts[3], 112, 1)
        for s in (2, 1, 0):
            out = jnp.where(lanes < 32 * (s + 1), pltpu.roll(parts[s], 32 * s + 16, 1), out)
        return out

    def gather(rows):
        return [ref[rows, :] for ref in E + H] + [pack([ref[rows, :] for ref in PZ])]

    def scatter(rows, values):
        for ref, value in zip(E + H, values):
            ref[rows, :] = value
        for s, ref in enumerate(PZ):
            ref[rows, :] = pltpu.roll(values[6], 112 - 32 * s, 1)

    def end_rows(d, layer, end, low):
        if low is None:
            place = layer if DIRS[d][d // 2] < 0 else 31 - layer
        else:
            place = -1 - layer if DIRS[d][d // 2] < 0 else 32 + layer
        if d < 2:
            return pl.ds(at(place, 30 * end) + zero, 2)
        return pl.ds(at(30 * end, place) + zero, 2, stride=YP)

    def face_copy(d, blk, start, n, k, incoming):
        span = pl.ds(start, n)
        to = d if incoming else OPP[d]
        return remote(
            d, send_f[d].at[span], recv_f[to].at[blk, span], s_sem.at[d, k], r_sem.at[blk, to, k]
        )

    def send_layer(d, layer, blk):
        buf = send_f[d]
        for q in range(4):
            for k, value in enumerate(gather(layer_rows(d, layer, q, None))):
                buf[pl.ds(pl.multiple_of(layer * LAYER + k * 32 + q * 8, 8), 8), :] = value
        guarded(d, face_copy(d, blk, pl.multiple_of(layer * LAYER, 8), LAYER, layer, False))

    extra_fields = {1: (H[1], H[2]), 3: (H[2], H[0])}
    tail_rows = lambda d: (FACE if d in (1, 3) else EXTRA) - ENDS

    def send_tail(d, blk):
        buf = send_f[d]
        for layer in range(2):
            for end in range(2):
                for k, value in enumerate(gather(end_rows(d, D + layer, end, None))):
                    s = ENDS + layer * NA * 4 + k * 4 + end * 2
                    buf[s : s + 2, :] = value
        if d in extra_fields:
            for k, ref in enumerate(extra_fields[d]):
                for q in range(4):
                    s = EXTRA + k * 32 + q * 8
                    buf[s : s + 8, :] = ref[layer_rows(d, D, q, None), :]
        guarded(d, face_copy(d, blk, ENDS, tail_rows(d), D, False))

    def send_corner(d, blk):
        buf, (dx, dy) = send_c[d - 4], DIRS[d]
        for i, (first, n) in enumerate(CORNER_ROWS):
            x = i if dx < 0 else 31 - i
            rows = pl.ds(at(x, 0 if dy < 0 else 32 - n) + zero, n)
            for k, value in enumerate(gather(rows)):
                buf[k * 8 + first : k * 8 + first + n, :] = value
        copy = remote(
            d, buf, recv_c[OPP[d] - 4].at[blk], s_sem.at[d, 0], r_sem.at[blk, OPP[d], 0]
        )
        guarded(d, copy)

    def edge_rows(d, layer, low):
        if low is None:
            place = layer if DIRS[d][d // 2] < 0 else 31 - layer
        else:
            place = -1 - layer if DIRS[d][d // 2] < 0 else 32 + layer
        if d < 2:
            return [pl.ds((place + XO) * PYP + 4 + 8 * q + zero, 8) for q in range(2)]
        return [pl.ds((8 * q + PXO) * YP + YO + place + zero, 8, stride=YP) for q in range(2)]

    def send_edge(d, blk):
        @pl.when(jnp.logical_and(exists[d], y_edge if d < 2 else x_edge))
        def _():
            buf = send_e[d]
            for layer in range(D):
                for k, ref in enumerate(PY if d < 2 else PX):
                    for q, rows in enumerate(edge_rows(d, layer, None)):
                        s = layer * 64 + k * 16 + q * 8
                        buf[s : s + 8, :] = ref[rows, :]
            remote(
                d, buf, recv_e[OPP[d]].at[blk], s_sem.at[d, D + 1], r_sem.at[blk, OPP[d], D + 1]
            ).start()

    def receive_face(d, blk):
        @pl.when(exists[d])
        def _():
            buf = recv_f[d]
            for k in range(D + 1):
                start, size = (k * LAYER, LAYER) if k < D else (ENDS, tail_rows(d))
                face_copy(d, blk, start, size, k, True).wait_send()
                if k == D:
                    size = tail_rows(OPP[d])
                face_copy(d, blk, start, size, k, True).wait_recv()

            def unpack(layer, c):
                for q in range(4):
                    scatter(
                        layer_rows(d, layer, q, True),
                        [
                            buf[blk, pl.ds(pl.multiple_of(layer * LAYER + k * 32 + q * 8, 8), 8), :]
                            for k in range(NA)
                        ],
                    )
                return c

            lax.fori_loop(0, D, unpack, 0)
            for layer in range(2):
                for end in range(2):
                    s = ENDS + layer * NA * 4 + end * 2
                    scatter(
                        end_rows(d, D + layer, end, True),
                        [buf[blk, s + 4 * k : s + 4 * k + 2, :] for k in range(NA)],
                    )
            if OPP[d] in extra_fields:
                for k, ref in enumerate(extra_fields[OPP[d]]):
                    for q in range(4):
                        s = EXTRA + k * 32 + q * 8
                        ref[layer_rows(d, D, q, True), :] = buf[blk, s : s + 8, :]

    def receive_corner(d, blk):
        @pl.when(exists[d])
        def _():
            buf, (dx, dy) = recv_c[d - 4], DIRS[d]
            copy = remote(d, send_c[d - 4], buf.at[blk], s_sem.at[d, 0], r_sem.at[blk, d, 0])
            copy.wait_recv()
            copy.wait_send()
            for i, (first, n) in enumerate(CORNER_ROWS):
                x = -1 - i if dx < 0 else 32 + i
                s = lambda k: k * 8 + first
                scatter(
                    pl.ds(at(x, -n if dy < 0 else 32) + zero, n),
                    [buf[blk, s(k) : s(k) + n, :] for k in range(NA)],
                )

    def receive_edge(d, blk):
        @pl.when(jnp.logical_and(exists[d], y_edge if d < 2 else x_edge))
        def _():
            buf = recv_e[d]
            copy = remote(d, send_e[d], buf.at[blk], s_sem.at[d, D + 1], r_sem.at[blk, d, D + 1])
            copy.wait_recv()
            copy.wait_send()
            for layer in range(D):
                for k, ref in enumerate(PY if d < 2 else PX):
                    for q, rows in enumerate(edge_rows(d, layer, True)):
                        s = layer * 64 + k * 16 + q * 8
                        ref[rows, :] = buf[blk, s : s + 8, :]

    for d in range(4):
        for layer in range(M):
            for q in range(4):
                s = layer * 32 + q * 8
                send_m[d][s : s + 8, :] = MF[layer_rows(d, layer, q, None), :]
        guarded(d, remote(d, send_m[d], recv_m[OPP[d]], sm_sem.at[d], rm_sem.at[OPP[d]]))
    for d in range(4, 8):
        dx, dy = DIRS[d]
        for i in range(M):
            rows = pl.ds(at(i if dx < 0 else 31 - i, 0 if dy < 0 else 28) + zero, 4)
            send_mc[d - 4][i * 4 : i * 4 + 4, :] = MF[rows, :]
        guarded(
            d, remote(d, send_mc[d - 4], recv_mc[OPP[d] - 4], sm_sem.at[d], rm_sem.at[OPP[d]])
        )

    def receive_material():
        for x in (0, 1, 2, 3, 4, 37, 38, 39, 40, 41):
            for k in range(6):
                MF[x * YP + k * 8 : x * YP + k * 8 + 8, :] = zeros

        def clear_side(x, c):
            MF[pl.ds(pl.multiple_of((x + XO) * YP, 8), 8), :] = zeros
            MF[pl.ds(pl.multiple_of((x + XO) * YP + 40, 8), 8), :] = zeros
            return c

        lax.fori_loop(0, 32, clear_side, 0)
        for d in range(8):

            @pl.when(exists[d])
            def _(d=d):
                dx, dy = DIRS[d]
                if d < 4:
                    copy = remote(d, send_m[d], recv_m[d], sm_sem.at[d], rm_sem.at[d])
                else:
                    copy = remote(d, send_mc[d - 4], recv_mc[d - 4], sm_sem.at[d], rm_sem.at[d])
                copy.wait_recv()
                copy.wait_send()
                for i in range(M):
                    if d < 4:
                        for q in range(4):
                            s = i * 32 + q * 8
                            MF[layer_rows(d, i, q, True), :] = recv_m[d][s : s + 8, :]
                    else:
                        x = -1 - i if dx < 0 else 32 + i
                        rows = pl.ds(at(x, -4 if dy < 0 else 32) + zero, 4)
                        MF[rows, :] = recv_mc[d - 4][i * 4 : i * 4 + 4, :]

        all_coefficients(-4, 0, (-4, 4, 12, 20, 28))
        all_coefficients(32, 36, (-4, 4, 12, 20, 28))
        all_coefficients(0, 32, (-4, 28))

    def table(tab, half, k, start, n):
        return tab[pl.ds(half * 3 * n + k * n + start, 8), :]

    def half_step(half, x0, size, starts, mask_of, px, py):
        source, target = (E, H) if half == 0 else (H, E)
        step = 1 if half == 0 else -1
        zc = [ztab[(half * 3 + k) * 8 : (half * 3 + k) * 8 + 8, :] for k in range(3)]
        keep_lane = lane < 127 if half == 0 else lane > 0
        for r in range(size):
            x = x0 + r
            if px:
                xc = [
                    jnp.broadcast_to(xtab[pl.ds((half * 3 + k) * 48 + x + XO, 1), :], (8, 128))
                    for k in range(3)
                ]
            for i, y in enumerate(starts):
                rows = lambda dx, dy: pl.ds(at(x + dx, y + dy) + zero, 8)
                here = rows(0, 0)
                mask = mask_of(r, x, i)

                def put(ref, where, value):
                    pltpu.store(ref.at[where, :], value, mask=mask)

                def diff(a, b):
                    return a - b if half == 0 else b - a

                s0, s1, s2 = (ref[here, :] for ref in source)
                sh = 127 if half == 0 else 1
                turn = lambda v: jnp.where(keep_lane, pltpu.roll(v, sh, 1), 0.0)
                dz1, dz0 = diff(turn(s1), s1), diff(turn(s0), s0)
                dy2 = diff(source[2][rows(0, step), :], s2)
                dy0 = diff(source[0][rows(0, step), :], s0)
                dx2 = diff(source[2][rows(step, 0), :], s2)
                dx1 = diff(source[1][rows(step, 0), :], s1)

                def term(d, coef, ref, where):
                    b, a, q = coef
                    new = b * ref[where, :] + a * d
                    put(ref, where, new)
                    return q * d + new

                tz1 = term(dz1, zc, PZ[2 * half], here)
                tz0 = term(dz0, zc, PZ[2 * half + 1], here)
                if px:
                    there = pl.ds((x - pxbase + PXO) * YP + YO + y + zero, 8)
                    tx2 = term(dx2, xc, PX[2 * half], there)
                    tx1 = term(dx1, xc, PX[2 * half + 1], there)
                else:
                    tx2, tx1 = dx2, dx1
                if i in py:
                    yc = [
                        ytab[pl.ds((half * 3 + k) * 48 + YO + y + zero, 8), :] for k in range(3)
                    ]
                    there = pl.ds((x + XO) * PYP + (y - py[i]) + zero, 8)
                    ty2 = term(dy2, yc, PY[2 * half], there)
                    ty0 = term(dy0, yc, PY[2 * half + 1], there)
                else:
                    ty2, ty0 = dy2, dy0
                curls = (ty2 - tz1, tz0 - tx2, tx1 - ty0)
                if half == 0:
                    for ref, c in zip(target, curls):
                        put(ref, here, ref[here, :] - time_step * c)
                else:
                    kp, dr = KP[here, :], DR[here, :]
                    for ref, c in zip(target, curls):
                        put(ref, here, kp * ref[here, :] + dr * c)

    px0 = jnp.where(x_first, 0, jnp.where(x_last, 16, -32))
    px1 = jnp.where(x_edge, px0 + 16, -32)

    def groups(half, xs, xe, size, starts, mask_of, py):
        over = lambda v: (v + 64) // size - 64 // size
        n = over(xe - xs + size - 1)
        ia = jnp.clip(over(px0 - xs), 0, n)
        ib = jnp.clip(over(px1 - xs + size - 1), 0, n)

        def plain(part, c):
            def one(i, c):
                half_step(half, xs + size * i, size, starts, mask_of, False, py)
                return c

            return lax.fori_loop(jnp.where(part == 0, 0, ib), jnp.where(part == 0, ia, n), one, c)

        lax.fori_loop(0, 2, plain, 0)

        def layered(i, c):
            half_step(half, xs + size * i, size, starts, mask_of, True, py)
            return c

        lax.fori_loop(ia, ib, layered, 0)

    def by_place(run, low, high):
        @pl.when(y_first)
        def _():
            run({i: -4 for i in low})

        @pl.when(y_last)
        def _():
            run({i: 12 for i in high})

        @pl.when(jnp.logical_not(y_edge))
        def _():
            run({})

    def inner_range(t, half, first, last):
        lo = jnp.where(first, 0, t - 1 + half)
        hi = jnp.where(last, 32, 32 - t)
        return lo, hi

    def within(v, lo, hi):
        return jnp.logical_and(v >= lo, v < hi)

    starts_a = (0, 8, 16, 24)
    starts_b = (-4, 4, 12, 20, 28)

    def pass_a(t, py):
        for half in range(2):
            xlo, xhi = inner_range(t, half, x_first, x_last)
            ylo, yhi = inner_range(t, half, y_first, y_last)

            def mask_of(r, x, i, xlo=xlo, xhi=xhi, ylo=ylo, yhi=yhi):
                ok = within(x, xlo, xhi).astype(jnp.int32)
                if i in (0, 3):
                    return within(row + starts_a[i], ylo, jnp.where(ok > 0, yhi, -99))
                return row >= 8 - 8 * ok

            groups(half, xlo, xhi, UA, starts_a, mask_of, py)

    def pass_b(t):
        ya = jnp.where(y_first, 0, -99)
        yb = jnp.where(y_last, 32, 99)
        for half in range(2):
            xc, xd = inner_range(t, half, x_first, x_last)
            yc, yd = inner_range(t, half, y_first, y_last)
            grow = t - 1 + half
            xa = jnp.where(x_first, 0, -t)
            xb = jnp.where(x_last, 32, 32 + grow)
            wa = jnp.where(y_first, 0, -t)
            wb = jnp.where(y_last, 32, 32 + grow)
            low = jnp.maximum(-t, t - 5 + half)
            high = 32 - t
            xs = jnp.where(x_first, 0, low + U)
            xe = jnp.where(x_last, 32, high)

            def mask_of(r, x, i, xa=xa, xb=xb, xc=xc, xd=xd, yc=yc, yd=yd, wa=wa, wb=wb):
                border = jnp.logical_or(within(x, xa, xc), within(x, xd, xb))
                if i not in (0, 4):
                    return row >= 8 - 8 * border.astype(jnp.int32)
                y = row + starts_b[i]
                if i == 0:
                    return within(y, jnp.where(border, ya, wa), jnp.where(border, 99, yc))
                return within(y, jnp.where(border, -99, yd), jnp.where(border, yb, wb))

            def ends_mask(r, x, i, yc=yc, yd=yd, wa=wa, wb=wb, xe=xe):
                y = row + (-4 if i == 0 else 28)
                if i == 0:
                    return within(y, wa, jnp.where(x < xe, yc, -99))
                return within(y, yd, jnp.where(x < xe, wb, -99))

            def borders(py, half=half, low=low, high=high, mask_of=mask_of):
                def border(p, c):
                    x0 = jnp.where(p == 0, low, high)
                    half_step(half, x0, U, starts_b, mask_of, False, py)
                    return c

                lax.fori_loop(jnp.where(x_first, 1, 0), jnp.where(x_last, 1, 2), border, 0)

            by_place(borders, (0, 1, 2), (2, 3, 4))
            groups(half, xs, xe, UE, (-4, 28), ends_mask, {})

            def outside_mask(r, x, i, low=low, yc=yc, yd=yd, wa=wa, wb=wb):
                y = row + (-4 if i == 0 else 28)
                if i == 0:
                    return within(y, wa, jnp.where(x < low, yc, -99))
                return within(y, yd, jnp.where(x < low, wb, -99))

            @pl.when(jnp.logical_and(jnp.logical_not(x_first), low + 5 - t - half > 0))
            def _(half=half, outside_mask=outside_mask):
                half_step(half, t - 5 + half, U, (-4, 28), outside_mask, False, {})

    def block(turn, c):
        blk = turn % 2

        def step_a(t, c):
            @pl.when(t <= D)
            def _():
                send_layer(1, t - 1, blk)
                send_layer(3, t - 1, blk)

            by_place(lambda py: pass_a(t, py), (0, 1), (2, 3))

            @pl.when(t == D)
            def _():
                for d in range(4, 8):
                    send_corner(d, blk)

            @pl.when(t <= D)
            def _():
                send_layer(0, t - 1, blk)
                send_layer(2, t - 1, blk)

            @pl.when(t == D)
            def _():
                for d in range(4):
                    send_tail(d, blk)
                for d in range(4):
                    send_edge(d, blk)

            return c

        lax.fori_loop(1, M + 1, step_a, 0)

        @pl.when(turn == 0)
        def _():
            receive_material()

        for d in range(4, 8):
            receive_corner(d, blk)
        for d in range(4):
            receive_edge(d, blk)
        for d in (2, 3, 0, 1):
            receive_face(d, blk)

        def step_b(t, c):
            pass_b(t)
            return c

        lax.fori_loop(1, M + 1, step_b, 0)
        return c

    lax.fori_loop(0, STEPS // M, block, 0)


def solution(mesh):
    nx, ny = mesh.shape["gx"], mesh.shape["gy"]
    f32 = jnp.float32
    field = P(None, "gx", "gy", None)

    def shards(e_field, h_field, psi, material, eps_table, sigma_table):
        big = pltpu.VMEM((XR * YP, 128), f32)
        dma = pltpu.SemaphoreType.DMA
        kept = [(XR * YP, 128)] * 10 + [(PXR * YP, 128)] * 4 + [(XR * PYP, 128)] * 4
        scratch = [big, big, big, pltpu.VMEM((1024, 128), jnp.int32)]
        scratch += [pltpu.VMEM((6 * 48, 128), f32)] * 2 + [pltpu.VMEM((48, 128), f32)]
        scratch += [pltpu.VMEM((FACE, 128), f32)] * 4 + [pltpu.VMEM((2, FACE, 128), f32)] * 4
        scratch += [pltpu.VMEM((CORNER, 128), f32)] * 4 + [pltpu.VMEM((2, CORNER, 128), f32)] * 4
        scratch += [pltpu.VMEM((EDGE, 128), f32)] * 4 + [pltpu.VMEM((2, EDGE, 128), f32)] * 4
        scratch += [pltpu.VMEM((128, 128), f32)] * 8 + [pltpu.VMEM((16, 128), f32)] * 8
        scratch += [
            dma((20,)),
            dma((8, D + 2)),
            dma((2, 8, D + 2)),
            dma((8,)),
            dma((8,)),
        ]
        anywhere = pl.BlockSpec(memory_space=pl.ANY)
        smem = pl.BlockSpec(memory_space=pltpu.SMEM)
        vmem = pl.BlockSpec(memory_space=pltpu.VMEM)
        state = pl.pallas_call(
            functools.partial(kernel, nx, ny),
            out_shape=[pltpu.VMEM(shape, f32) for shape in kept],
            in_specs=[anywhere] * 4 + [smem] * 2,
            out_specs=[vmem] * len(kept),
            scratch_shapes=scratch,
            compiler_params=pltpu.CompilerParams(
                collective_id=0, has_side_effects=True, vmem_limit_bytes=40 << 20
            ),
        )(e_field, h_field, psi, material.reshape(1024, 128), eps_table, sigma_table)
        state = [pltpu.with_memory_space_constraint(a, pltpu.VMEM) for a in state]
        return pl.pallas_call(
            functools.partial(store_kernel, nx, ny),
            out_shape=[jax.ShapeDtypeStruct(a.shape, f32) for a in (e_field, h_field, psi)],
            in_specs=[vmem] * len(kept),
            out_specs=[anywhere] * 3,
            scratch_shapes=[pltpu.VMEM((1024, 128), f32), dma((10,)), dma((2, 8))],
            compiler_params=pltpu.CompilerParams(vmem_limit_bytes=8 << 20),
        )(*state)

    return jax.shard_map(
        shards,
        mesh=mesh,
        in_specs=(field, field, field, P("gx", "gy", None), P(), P()),
        out_specs=(field, field, field),
        check_vma=False,
    )
```
